512 devices in a mesh: groups: 2 (over y), seq: 16 (over z), fsdp: 8 (over x), sub: 2 (over core).
Axes of the slice: x: 8, y: 2, z: 16, core: 2. Of those that a mesh axis runs over, the one named last changes fastest.
The devices are a block of a 8x8x16 slice.
Arguments:
- tokens: bfloat16 [8192, 8192], P(('groups', 'seq')), parts along dimension 0, may hold values from -400 to 400
- norm_gain: float32 [8192], replicated, may hold values from 0.1 to 1.9
- w_query: bfloat16 [32, 16, 8192], P(('seq', 'sub'), 'fsdp'), may hold values from -0.0625 to 0.0625
- w_key: bfloat16 [32, 16, 8192], P(('seq', 'sub'), 'fsdp'), may hold values from -0.0625 to 0.0625
- w_value: bfloat16 [32, 128, 8192], P(('seq', 'sub'), 'fsdp'), may hold values from -5 to 5
- head_gain: float32 [128], replicated, may hold values from 0.1 to 1.9
- w_out: bfloat16 [32, 128, 8192], P('seq', None, ('fsdp', 'sub')), may hold values from -0.09375 to 0.09375
Outputs:
- mixed: bfloat16 [8192, 8192], P(('groups', 'seq'), ('fsdp', 'sub')), parts along dimension 0
The draws below stay inside these ranges and needn't reach their ends.
There are 2 independent parts, one for each index of `groups`. The reference program is written for one: setup_inputs(seed, part) draws one part's arguments, and reference() takes and returns one part's arrays. A program takes and returns all parts, laid end to end along the dimension named above; an argument that names none is the same for every part. Nothing has to cross between parts.
All inputs are finite; a program needn't handle non-finite values.
Results may differ from the reference program's by a relative error of at most 0.0084.
Values may be sent and summed in bfloat16 or wider, within the bound.
A program may use at most 64 MiB of HBM per device.

```python
import math
import jax
import jax.numpy as jnp
import numpy as np
from jax import lax

D = 8192
HEAD_DIM = 128
FEAT = 16
BLOCK = 512
HEADS = 32
L = 4096


def draw_tokens(key, part):
    subkeys = jax.random.split(jax.random.fold_in(key, 101), 3)
    row_scale = jnp.exp(jax.random.uniform(subkeys[0], (L, 1), jnp.float32, 0.0, math.log(10.0)))
    col_scale = jnp.exp(jax.random.uniform(subkeys[1], (1, D), jnp.float32, 0.0, math.log(10.0)))
    entries = jnp.clip(jax.random.normal(subkeys[2], (L, D), jnp.float32), -4.0, 4.0)
    return (entries * row_scale * col_scale).astype(jnp.bfloat16)


def draw_w_value(key, part):
    subkeys = jax.random.split(jax.random.fold_in(key, 202), 2)
    upward = jnp.arange(HEAD_DIM, dtype=jnp.float32)[None, :, None] / (HEAD_DIM - 1.0)
    jitter = jax.random.uniform(subkeys[0], (HEADS, HEAD_DIM, 1), jnp.float32, 0.0, 1.0)
    exponent = 0.5 * upward + 0.5 * jitter
    entries = jnp.clip(jax.random.normal(subkeys[1], (HEADS, HEAD_DIM, D), jnp.float32), -4.0, 4.0)
    factor = jnp.power(10.0, exponent) / math.sqrt(D)
    return (entries * factor).astype(jnp.bfloat16)


def levels(key, extent, cuts, low, top_value):
    gain, own = 1.0, jax.random.fold_in(key, 6)
    for position, parts in cuts:
        draws = jnp.exp(jax.random.uniform(jax.random.fold_in(own, position), (parts,), jnp.float32, low / len(cuts), top_value / len(cuts)))
        gain = gain * jnp.repeat(draws, extent[position] // parts).reshape([-1 if axis == position else 1 for axis in range(len(extent))])
    return gain


def centred(own_key, dims, width, limit, cuts=(), kind=jnp.bfloat16):
    drawn = jax.random.normal(own_key, dims, jnp.float32) * width
    if len(cuts) > 0:
        drawn = levels(own_key, dims, cuts, -0.22, 0.18) * drawn
    return jnp.clip(drawn, min=-limit, max=limit).astype(kind)


def setup_inputs(seed: int = 0, part: int = 0) -> dict:
    key_list = jax.random.split(jax.random.key(seed), 8)
    own_keys = jax.random.split(jax.random.fold_in(key_list[7], part), 8)
    tokens = draw_tokens(jax.random.fold_in(jax.random.fold_in(key_list[7], part), 71), part)
    norm_gain = jnp.clip(1.0 + 0.18 * jax.random.normal(key_list[1], (D,), jnp.float32), 0.1, 1.9)
    w_query = centred(key_list[2], (HEADS, FEAT, D), D ** -0.5, 0.0625, ((0, 32), (1, 8)))
    w_key = centred(key_list[3], (HEADS, FEAT, D), D ** -0.5, 0.0625, ((0, 32), (1, 8)))
    w_value = draw_w_value(jax.random.fold_in(key_list[7], 71), part)
    head_gain = jnp.clip(1.0 + 0.18 * jax.random.normal(key_list[5], (HEAD_DIM,), jnp.float32), 0.1, 1.9)
    w_out = centred(key_list[6], (HEADS, HEAD_DIM, D), (HEADS * HEAD_DIM) ** -0.5, 0.09375, ((0, 16), (2, 16)))
    return dict(tokens=tokens, norm_gain=norm_gain, w_query=w_query, w_key=w_key, w_value=w_value, head_gain=head_gain, w_out=w_out)


def taylor_last(vectors):
    feature_count = vectors.shape[-1]
    first_row, second_row = np.triu_indices(feature_count, 1)
    cross_terms = vectors[..., first_row] * vectors[..., second_row] / 4.0
    squares = vectors * vectors / (4.0 * math.sqrt(2.0))
    leading = jnp.ones(vectors.shape[:-1] + (1,), jnp.float32)
    return jnp.concatenate([leading, vectors / 2.0, cross_terms, squares], -1)

def reference(tokens, norm_gain, w_query, w_key, w_value, head_gain, w_out):
    inputs = tokens.astype(jnp.float32)
    meansq = lax.optimization_barrier(jnp.mean(inputs * inputs, axis=-1, keepdims=True))
    normed = (inputs * lax.rsqrt(meansq + 1e-05) * norm_gain).astype(jnp.bfloat16)
    length = tokens.shape[0]

    def project(weight):
        flattened = weight.reshape(-1, weight.shape[-1])
        result = jnp.dot(normed, flattened.T, preferred_element_type=jnp.float32)
        result = result.astype(jnp.bfloat16).reshape(length, weight.shape[0], weight.shape[1])
        return jnp.transpose(result, (1, 0, 2))
    queries = project(w_query)
    key_vectors = project(w_key)
    values_all = project(w_value)
    nblocks = length // BLOCK
    position_t = jnp.arange(BLOCK, dtype=jnp.int32)[:, None]
    position_j = jnp.arange(BLOCK, dtype=jnp.int32)[None, :]
    causal = position_j <= position_t

    def one_head(operands):
        head_query, head_key, head_value = operands
        query_feats = taylor_last(head_query.astype(jnp.float32)).astype(jnp.bfloat16)
        key_feats = taylor_last(head_key.astype(jnp.float32)).astype(jnp.bfloat16)
        key_blocks = key_feats.astype(jnp.float32).reshape(nblocks, BLOCK, -1)
        value_blocks = head_value.astype(jnp.float32).reshape(nblocks, BLOCK, -1)
        contrib = jnp.einsum('bjf,bje->bfe', key_blocks, value_blocks)
        prefix = jnp.concatenate([jnp.zeros_like(contrib[:1]), jnp.cumsum(contrib[:-1], axis=0)], 0)
        prior_state = prefix.astype(jnp.bfloat16)
        query_blocks = head_query.astype(jnp.float32).reshape(nblocks, BLOCK, -1)
        raw_keys = head_key.astype(jnp.float32).reshape(nblocks, BLOCK, -1)
        scores = jnp.einsum('btf,bjf->btj', query_blocks, raw_keys)
        kernel = 1.0 + scores / 4.0 + scores * scores / 32.0
        weight = jnp.where(causal[None], kernel, 0.0).astype(jnp.bfloat16)
        local_part = jnp.einsum('btj,bje->bte', weight.astype(jnp.float32), value_blocks)
        feat_blocks = query_feats.astype(jnp.float32).reshape(nblocks, BLOCK, -1)
        carried = jnp.einsum('btf,bfe->bte', feat_blocks, prior_state.astype(jnp.float32))
        return (local_part + carried).reshape(length, -1).astype(jnp.bfloat16)
    numerator = lax.map(one_head, (queries, key_vectors, values_all))
    widened = numerator.astype(jnp.float32)
    meansq_out = lax.optimization_barrier(jnp.mean(widened * widened, axis=-1, keepdims=True))
    attended = (widened * lax.rsqrt(meansq_out + 1e-06) * head_gain).astype(jnp.bfloat16)
    flat_att = jnp.transpose(attended, (1, 0, 2)).reshape(length, -1)
    out_rows = w_out.reshape(-1, w_out.shape[-1])
    return jnp.dot(flat_att, out_rows, preferred_element_type=jnp.float32).astype(jnp.bfloat16)
```

```python
import functools

import jax
import jax.numpy as jnp
import numpy as np
from jax import lax
from jax.experimental import pallas as pl
from jax.experimental.pallas import tpu as pltpu
from jax.sharding import PartitionSpec as P

BLOCK = 512
LANES = 128
STATE_ROWS = 160
MESH = pl.DeviceIdType.MESH
bf16, f32 = jnp.bfloat16, jnp.float32


def feature_tables(owners, dims):
    count = owners * dims
    tables = np.zeros((2, 4, LANES, 2 * LANES), np.float32)
    bias = np.zeros((8, 2 * LANES), np.float32)
    for head in range(2):
        for kind in range(2):

            def entry(i):
                return (i // dims) * 4 * dims + head * 2 * dims + kind * dims + i % dims

            first, second = tables[head, 2 * kind], tables[head, 2 * kind + 1]
            for i in range(count):
                first[entry(i), i] = 0.5
            column = count + 1
            for i in range(count):
                for j in range(i, count):
                    first[entry(i), column] = 0.125 if (i == j and kind == 1) else 0.25
                    second[entry(j), column] = 1.0
                    column += 1
    bias[0, count] = 1.0
    bias[1, : count + 1] = 1.0
    return jnp.asarray(tables, bf16), jnp.asarray(bias, f32)


class Ring:
    def __init__(self, axis, size, me, piece, pieces, split, send, recv):
        self.axis, self.size, self.me = axis, size, me
        self.piece, self.pieces, self.split = piece, pieces, split
        self.send, self.recv, self.last = send, recv, size // 2

    def moves(self, way, step, p):
        return step < self.last or (p < self.split) == (way == 0)

    def block(self, way, back):
        return lax.rem(self.me + (self.size - back if way == 0 else back), self.size)

    def copy(self, way, step, p, block):
        to = lax.rem(self.me + (1 if way == 0 else self.size - 1), self.size)
        ref = self.piece(p, block)
        return pltpu.make_async_remote_copy(
            src_ref=ref,
            dst_ref=ref,
            send_sem=self.send.at[way, step - 1, p],
            recv_sem=self.recv.at[way, step - 1, p],
            device_id={self.axis: to},
            device_id_type=MESH,
        )

    def start(self, way, step, p):
        if step <= self.last and self.moves(way, step, p):
            self.copy(way, step, p, self.block(way, step - 1)).start()

    def first(self):
        for p in range(self.pieces):
            for way in range(2):
                self.start(way, 1, p)

    def tick(self, step, arrived=None):
        for p in range(self.pieces):
            for way in range(2):
                if self.moves(way, step, p):
                    self.copy(way, step, p, self.block(way, step)).wait_recv()
                    self.start(way, step + 1, p)
                    if arrived is not None:
                        arrived(way, step, p, self.block(way, step))

    def drain(self):
        for step in range(1, self.last + 1):
            for p in range(self.pieces):
                for way in range(2):
                    if self.moves(way, step, p):
                        self.copy(way, step, p, self.me).wait_send()


def nt(a, b):
    return lax.dot_general(a, b, (((1,), (1,)), ((), ())), preferred_element_type=f32)


def layer(S, X, tokens, gain, wq, wk, wv, hgain, wo, tab, bias, out,
          tokv, T, W, QKf, qkown, qkin, Pm, Rcv, Snd, Rx, tabv, Cown, Crecv, Sacc, Sp, num, A0, A1, Att, WO, acc,
          lsem, tS, tR, wS, wR, oS, oR, aS, aR, pS, pR, e2S, e2R, e3S, e3R, cS, cR, e4S, e4R, zS, zR, ownS, ownR, relS, relR):
    x, z, c = lax.axis_index("fsdp"), lax.axis_index("seq"), lax.axis_index("sub")
    R, D = tokv.shape
    Dh = D // 2
    vd, fd = wv.shape[0], wq.shape[0]
    HD = X * vd
    PB, Ppl = Rx.shape[0], Rx.shape[1]
    Bk = PB * Ppl
    other = 1 - c
    mine = pl.ds(pl.multiple_of(c * Dh, LANES), Dh)
    theirs = pl.ds(pl.multiple_of(other * Dh, LANES), Dh)

    def rows(i, n):
        return pl.ds(pl.multiple_of(i * n, n), n)

    def remote(src, dst, send, recv, **device):
        return pltpu.make_async_remote_copy(
            src_ref=src, dst_ref=dst, send_sem=send, recv_sem=recv, device_id=device, device_id_type=MESH)

    barrier = pltpu.get_barrier_semaphore()
    for k in range(1, S):
        pl.semaphore_signal(barrier, inc=1, device_id={"seq": lax.rem(z + k, S)}, device_id_type=MESH)
    for k in range(1, X):
        pl.semaphore_signal(barrier, inc=1, device_id={"fsdp": lax.rem(x + k, X)}, device_id_type=MESH)
    pl.semaphore_signal(barrier, inc=1, device_id={"sub": other}, device_id_type=MESH)

    get_tokens = pltpu.make_async_copy(tokens.at[rows(x, R)], tokv, lsem.at[0])
    get_value = pltpu.make_async_copy(wv.at[:, mine], W.at[rows(x, vd)], lsem.at[1])
    get_out = pltpu.make_async_copy(wo, WO.at[z], lsem.at[2])
    get_tab = pltpu.make_async_copy(tab.at[c], tabv, lsem.at[3])
    get_tokens.start()
    get_value.start()
    get_out.start()
    get_tab.start()

    W[2 * HD + 4 * fd * X :, :] = jnp.zeros((W.shape[0] - 2 * HD - 4 * fd * X, Dh), bf16)
    qkown[...] = jnp.zeros_like(qkown)
    for head in range(2):
        @pl.when(c == head)
        def _():
            base = 2 * fd * head
            qkown[base : base + fd, :] = wq[...].astype(f32)
            qkown[base + fd : base + 2 * fd, :] = wk[...].astype(f32)

    get_tokens.wait()
    chunk = min(1024, D)

    def squares(i, total):
        part = tokv[:, pl.ds(pl.multiple_of(i * chunk, chunk), chunk)].astype(f32)
        return total + jnp.sum(part * part, axis=1, keepdims=True)

    meansq = lax.fori_loop(0, D // chunk, squares, jnp.zeros((R, 1), f32)) / D
    scale = lax.rsqrt(meansq + 1e-05)
    chunk = min(1024, Dh)

    @pl.loop(0, Dh // chunk)
    def _(i):
        here = pl.ds(pl.multiple_of(c * Dh + i * chunk, chunk), chunk)
        part = tokv[:, here].astype(f32) * scale * gain[:, here]
        T[z, :, pl.ds(pl.multiple_of(i * chunk, chunk), chunk)] = part.astype(bf16)

    pl.semaphore_wait(barrier, S + X - 1)

    half = R // 2
    token_ring = Ring("seq", S, z, lambda p, b: T.at[b, half * p : half * (p + 1)], 2, 1, tS, tR)
    token_ring.first()

    give_value = remote(wv.at[:, theirs], W.at[pl.ds(pl.multiple_of(HD + x * vd, vd), vd)], pS.at[0], pR.at[0], sub=other)
    give_qk = remote(qkown.at[:, theirs], qkin, pS.at[1], pR.at[1], sub=other)
    give_value.start()
    give_qk.start()

    def weight_piece(p, b):
        if p == 2:
            return QKf.at[rows(b, 4 * fd)]
        return W.at[pl.ds(pl.multiple_of(HD * p + b * vd, vd), vd)]

    weight_ring = Ring("fsdp", X, x, weight_piece, 3, 1, wS, wR)
    get_value.wait()
    give_value.wait_recv()
    give_qk.wait_recv()
    QKf[rows(x, 4 * fd), :] = qkown[:, mine] + qkin[...]
    weight_ring.first()

    Oh = 2 * HD // 2
    out_ring = Ring("seq", S, z, lambda p, b: WO.at[b, Oh * p : Oh * (p + 1)], 2, 1, oS, oR)

    ticks = [(5.6 * s, 0, s) for s in range(1, S // 2 + 1)] + [(3.0 + 8.5 * s, 1, s) for s in range(1, X // 2 + 1)]
    for _, which, step in sorted(ticks):
        if which == 0:
            if step == S // 2:
                get_out.wait()
                out_ring.first()
            token_ring.tick(step)
        else:
            weight_ring.tick(step)

    W[2 * HD : 2 * HD + 4 * fd * X, :] = QKf[...].astype(bf16)
    group = min(4, S)

    @pl.loop(0, S // group)
    def _(i):
        lhs = T[pl.ds(i * group, group)].reshape(group * R, Dh)
        Pm[rows(i, group * R), :] = nt(lhs, W[...])

    swap = remote(Pm.at[:, HD : 2 * HD + LANES], Rcv, e2S.at[0], e2R.at[0], sub=other)
    swap.start()
    get_tab.wait()
    swap.wait_recv()
    Snd[:, :, :HD] = (Pm[:, :HD] + Rcv[:, :HD]).astype(bf16).reshape(S, R, HD)
    Snd[:, :, HD:] = (Pm[:, 2 * HD :] + Rcv[:, HD:]).astype(bf16).reshape(S, R, LANES)

    def to_block(k):
        to = lax.rem(x + k, X)
        return remote(Snd.at[pl.ds(to * PB, PB)], Rx.at[:, rows(x, R)], e3S.at[k], e3R.at[k], fsdp=to)

    for k in range(1, X):
        to_block(k).start()
    Rx[:, rows(x, R), :] = Snd[pl.ds(x * PB, PB)]
    out_ring.tick(1)
    for k in range(1, X):
        to_block(k).wait_recv()

    val = Rx[:, :, :HD].reshape(Bk, HD)
    qk = Rx[:, :, HD:].reshape(Bk, LANES)

    def factor(which):
        return jnp.dot(qk, tabv[which], preferred_element_type=f32)

    b1, b2 = bias[0:1, :], bias[1:2, :]
    key_feats = ((factor(2) + b1) * (factor(3) + b2)).astype(bf16)
    contrib = lax.dot_general(key_feats, val, (((0,), (0,)), ((), ())), preferred_element_type=f32)
    Cown[...] = contrib[:STATE_ROWS].astype(bf16)

    def to_later(k):
        return remote(Cown, Crecv.at[k], cS.at[k], cR.at[k], fsdp=lax.rem(x + k, X))

    for k in range(1, X):
        @pl.when(x + k < X)
        def _():
            to_later(k).start()

    query_feats = ((factor(0) + b1) * (factor(1) + b2)).astype(bf16)
    lane = lax.broadcasted_iota(jnp.int32, (Bk, LANES), 1)
    count = X * fd
    zero = jnp.zeros((Bk, LANES), bf16)
    line_q = jnp.where(lane <= count, query_feats[:, :LANES], zero)
    line_k = jnp.where(lane <= count, key_feats[:, :LANES], zero)
    tile = min(128, Bk)
    for i in range(Bk // tile):
        seen = (i + 1) * tile
        g = nt(line_q[i * tile : seen], line_k[:seen])
        at = i * tile + lax.broadcasted_iota(jnp.int32, (tile, seen), 0)
        key_at = lax.broadcasted_iota(jnp.int32, (tile, seen), 1)
        weight = jnp.where(key_at <= at, 0.5 * (g * g) + 0.5, 0.0).astype(bf16)
        num[i * tile : seen, :] = jnp.dot(weight, val[:seen], preferred_element_type=f32)

    Sacc[...] = jnp.zeros_like(Sacc)
    for k in range(1, X):
        @pl.when(x >= k)
        def _():
            to_later(k).wait_recv()
            Sacc[...] += Crecv[k].astype(f32)

    Sp[STATE_ROWS:, :] = jnp.zeros((2 * LANES - STATE_ROWS, HD), bf16)
    Sp[:STATE_ROWS, :] = Sacc[...].astype(bf16)
    numerator = num[...] + jnp.dot(query_feats, Sp[...], preferred_element_type=f32)
    widened = numerator.astype(bf16).astype(f32)
    power = jnp.mean(widened * widened, axis=1, keepdims=True)
    attended = (widened * lax.rsqrt(power + 1e-06) * hgain[...]).astype(bf16)
    A0[...] = attended.reshape(PB, Ppl, HD)

    def to_share(k):
        to = lax.rem(x + k, X)
        return remote(A0.at[:, rows(to, R)], A1.at[pl.ds(x * PB, PB)], e4S.at[k], e4R.at[k], fsdp=to)

    for k in range(1, X):
        to_share(k).start()
    A1[pl.ds(x * PB, PB)] = A0[:, rows(x, R), :]
    out_ring.tick(2)
    for k in range(1, X):
        to_share(k).wait_recv()

    lanes = pl.ds(pl.multiple_of(c * HD, LANES), HD)

    def to_plane(k):
        to = lax.rem(z + k, S)
        return remote(A1.at[to], Att.at[z, rows(x, R), lanes], zS.at[k], zR.at[k], seq=to)

    for k in range(1, S):
        to_plane(k).start()
    Att[z, rows(x, R), lanes] = A1[z]
    for step in range(3, S // 2 - 3):
        out_ring.tick(step)
    for k in range(1, S):
        to_plane(k).wait_recv()

    upper = S // 2

    def share(p, b):
        return Att.at[upper * p : upper * (p + 1), rows(b, R), lanes]

    def relay(way, step, p, b):
        return remote(share(p, b), share(p, b), relS.at[way, step - 1, p], relR.at[way, step - 1, p], sub=other)

    def own_relay(p):
        return remote(share(p, x), share(p, x), ownS.at[p], ownR.at[p], sub=other)

    share_ring = Ring("fsdp", X, x, share, 2, 1, aS, aR)
    share_ring.first()
    for p in range(2):
        own_relay(p).start()
    done = max(S // 2 - 4, 2)
    for step in range(1, X // 2 + 1):
        share_ring.tick(step, lambda way, s, p, b: relay(way, s, p, b).start())
        if step == 2 and S // 2 > 4:
            done += 1
            out_ring.tick(done)

    other_lanes = pl.ds(pl.multiple_of(other * HD, LANES), HD)
    for p in range(2):
        own_relay(p).wait_recv()
    for step in range(1, X // 2 + 1):
        for p in range(2):
            for way in range(2):
                if share_ring.moves(way, step, p):
                    relay(way, step, p, share_ring.block(way, step)).wait_recv()

    acc[...] = jnp.dot(Att[z], WO[z], preferred_element_type=f32)

    def add(b):
        acc[...] += jnp.dot(Att[b], WO[b], preferred_element_type=f32)

    @pl.loop(1, done + 1)
    def _(s):
        add(lax.rem(z + s, S))

        @pl.when(s < S // 2)
        def _():
            add(lax.rem(z + S - s, S))

    for step in range(done + 1, S // 2 + 1):
        out_ring.tick(step)
        add(lax.rem(z + step, S))
        if step < S // 2:
            add(lax.rem(z + S - step, S))
    out[...] = acc[...].astype(bf16)

    token_ring.drain()
    weight_ring.drain()
    out_ring.drain()
    share_ring.drain()
    give_value.wait_send()
    give_qk.wait_send()
    swap.wait_send()
    for k in range(1, X):
        to_block(k).wait_send()
        to_share(k).wait_send()

        @pl.when(x + k < X)
        def _():
            to_later(k).wait_send()
    for k in range(1, S):
        to_plane(k).wait_send()
    for p in range(2):
        own_relay(p).wait_send()
    for step in range(1, X // 2 + 1):
        for p in range(2):
            for way in range(2):
                if share_ring.moves(way, step, p):
                    relay(way, step, p, x).wait_send()


def solution(mesh):
    S, X = mesh.shape["seq"], mesh.shape["fsdp"]

    def per_device(tokens, norm_gain, w_query, w_key, w_value, head_gain, w_out):
        Ppl, D = tokens.shape
        fd, vd = w_query.shape[1], w_value.shape[1]
        HD, R, Dh, C = X * vd, Ppl // X, D // 2, w_out.shape[2]
        PB = BLOCK // Ppl
        tab, bias = feature_tables(X, fd)
        any_ref = pl.BlockSpec(memory_space=pl.ANY)
        vm = pl.BlockSpec(memory_space=pltpu.VMEM)
        dma = pltpu.SemaphoreType.DMA
        V = pltpu.VMEM
        scratch = [
            V((R, D), bf16),
            V((S, R, Dh), bf16),
            V((2 * HD + LANES, Dh), bf16),
            V((4 * fd * X, Dh), f32),
            V((4 * fd, D), f32),
            V((4 * fd, Dh), f32),
            V((S * R, 2 * HD + LANES), f32),
            V((S * R, HD + LANES), f32),
            V((S, R, HD + LANES), bf16),
            V((PB, Ppl, HD + LANES), bf16),
            V((4, LANES, 2 * LANES), bf16),
            V((STATE_ROWS, HD), bf16),
            V((X, STATE_ROWS, HD), bf16),
            V((STATE_ROWS, HD), f32),
            V((2 * LANES, HD), bf16),
            V((PB * Ppl, HD), f32),
            V((PB, Ppl, HD), bf16),
            V((S, R, HD), bf16),
            V((S, Ppl, 2 * HD), bf16),
            V((S, 2 * HD, C), bf16),
            V((Ppl, C), f32),
            dma((4,)),
            dma((2, S // 2, 2)), dma((2, S // 2, 2)),
            dma((2, X // 2, 3)), dma((2, X // 2, 3)),
            dma((2, S // 2, 2)), dma((2, S // 2, 2)),
            dma((2, X // 2, 2)), dma((2, X // 2, 2)),
            dma((2,)), dma((2,)),
            dma((1,)), dma((1,)),
            dma((X,)), dma((X,)),
            dma((X,)), dma((X,)),
            dma((X,)), dma((X,)),
            dma((S,)), dma((S,)),
            dma((2,)), dma((2,)),
            dma((2, X // 2, 2)), dma((2, X // 2, 2)),
        ]
        return pl.pallas_call(
            functools.partial(layer, S, X),
            out_shape=jax.ShapeDtypeStruct((Ppl, C), bf16),
            in_specs=[any_ref, vm, vm, vm, any_ref, vm, any_ref, any_ref, vm],
            out_specs=vm,
            scratch_shapes=scratch,
            compiler_params=pltpu.CompilerParams(
                collective_id=0, has_side_effects=True, vmem_limit_bytes=48 * 1024 * 1024),
            name="layer",
        )(
            tokens,
            norm_gain.reshape(1, D),
            w_query.reshape(fd, D),
            w_key.reshape(fd, D),
            w_value.reshape(vd, D),
            head_gain.reshape(1, HD),
            w_out.reshape(2 * HD, C),
            tab,
            bias,
        )

    in_specs = (
        P(("groups", "seq"), None),
        P(),
        P(("seq", "sub"), "fsdp", None),
        P(("seq", "sub"), "fsdp", None),
        P(("seq", "sub"), "fsdp", None),
        P(),
        P("seq", None, ("fsdp", "sub")),
    )
    out_specs = P(("groups", "seq"), ("fsdp", "sub"))
    return jax.shard_map(
        per_device, mesh=mesh, in_specs=in_specs, out_specs=out_specs, check_vma=False
    )
```

```python
import functools

import jax
import jax.numpy as jnp
import numpy as np
from jax import lax
from jax.experimental import pallas as pl
from jax.experimental.pallas import tpu as pltpu
from jax.sharding import PartitionSpec as P

LANES = 128
FEATURES = 160
GROUP = 4
MESH = pl.DeviceIdType.MESH
bf16, f32 = jnp.bfloat16, jnp.float32


def feature_tables(owners, dims):
    count = owners * dims
    queries = np.zeros((2, 2, LANES, 2 * LANES), np.float32)
    pick = np.zeros((2, count, 4 * count), np.float32)
    keys = np.zeros((2, FEATURES, count), np.float32)
    bias = np.zeros((8, 2 * LANES), np.float32)

    def entry(i, head, kind):
        return (i // dims) * 4 * dims + head * 2 * dims + kind * dims + i % dims

    for i in range(count):
        keys[0, i, i] = 0.5
        for head in range(2):
            queries[head, 0, entry(i, head, 0), i] = 0.5
            pick[head, i, entry(i, head, 1)] = 1.0
    feature = count + 1
    for i in range(count):
        for j in range(i, count):
            keys[0, feature, i] = 0.125 if i == j else 0.25
            keys[1, feature, j] = 1.0
            for head in range(2):
                queries[head, 0, entry(i, head, 0), feature] = 0.25
                queries[head, 1, entry(j, head, 0), feature] = 1.0
            feature += 1
    bias[0, count] = 1.0
    bias[1, : count + 1] = 1.0
    upright = np.zeros((2, FEATURES, LANES), np.float32)
    upright[0], upright[1] = bias[0, :FEATURES, None], bias[1, :FEATURES, None]
    return (jnp.asarray(queries, bf16), jnp.asarray(pick, bf16), jnp.asarray(keys, bf16),
            jnp.asarray(bias, f32), jnp.asarray(upright, f32))


class Ring:
    def __init__(self, axis, size, me, piece, pieces, split, send, recv):
        self.axis, self.size, self.me = axis, size, me
        self.piece, self.pieces, self.split = piece, pieces, split
        self.send, self.recv, self.last = send, recv, size // 2

    def moves(self, way, step, p):
        return step < self.last or (p < self.split) == (way == 0)

    def block(self, way, back):
        return lax.rem(self.me + (self.size - back if way == 0 else back), self.size)

    def copy(self, way, step, p, src, dst):
        to = lax.rem(self.me + (1 if way == 0 else self.size - 1), self.size)
        return pltpu.make_async_remote_copy(
            src_ref=src,
            dst_ref=dst,
            send_sem=self.send.at[way, step - 1, p],
            recv_sem=self.recv.at[way, step - 1, p],
            device_id={self.axis: to},
            device_id_type=MESH,
        )

    def start(self, way, step, p):
        if step <= self.last and self.moves(way, step, p):
            block = self.block(way, step - 1)
            self.copy(way, step, p, self.piece(p, way, step - 1, block), self.piece(p, way, step, block)).start()

    def first(self, pieces=None):
        for p in range(self.pieces) if pieces is None else pieces:
            for way in range(2):
                self.start(way, 1, p)

    def tick(self, step, arrived=None):
        for p in range(self.pieces):
            for way in range(2):
                if self.moves(way, step, p):
                    block = self.block(way, step)
                    ref = self.piece(p, way, step, block)
                    self.copy(way, step, p, ref, ref).wait_recv()
                    self.start(way, step + 1, p)
                    if arrived is not None:
                        arrived(way, step, p, block)

    def drain(self):
        for step in range(1, self.last + 1):
            for p in range(self.pieces):
                for way in range(2):
                    if self.moves(way, step, p):
                        ref = self.piece(p, way, step - 1, self.me)
                        self.copy(way, step, p, ref, ref).wait_send()


def nt(a, b):
    return lax.dot_general(a, b, (((1,), (1,)), ((), ())), preferred_element_type=f32)


def mm(a, b):
    return jnp.dot(a, b, preferred_element_type=f32)


def slot_of(size, way, step):
    if step == 0:
        return 0
    return size - 1 if step == size // 2 else 2 * step - 1 + way


def layer(S, X, sets, tokens, gain, wq, wk, wv, hgain, wo, qtab, pick, ktab, bias, upright, out,
          tokv, T, W, QKf, qkown, qkin, Pn, Rn, PT, RT, Qn, Vp, Kg, VBD, Cs, Sg, Fq, num, A1, Att, WO, acc, qtabv, pickv,
          lsem, tS, tR, wS, wR, oS, oR, aS, aR, kS, kR, pS, pR, e2S, e2R, zS, zR, ownS, ownR, relS, relR):
    x, z, c = lax.axis_index("fsdp"), lax.axis_index("seq"), lax.axis_index("sub")
    R, D = tokv.shape
    Dh = D // 2
    vd, fd = wv.shape[0], wq.shape[0]
    HD = X * vd
    count = X * fd
    other = 1 - c
    mine = pl.ds(pl.multiple_of(c * Dh, LANES), Dh)
    theirs = pl.ds(pl.multiple_of(other * Dh, LANES), Dh)

    def rows(i, n):
        return pl.ds(pl.multiple_of(i * n, n), n)

    def remote(src, dst, send, recv, **device):
        return pltpu.make_async_remote_copy(
            src_ref=src, dst_ref=dst, send_sem=send, recv_sem=recv, device_id=device, device_id_type=MESH)

    barrier = pltpu.get_barrier_semaphore()
    greeted = [{"seq": lax.rem(z + 1, S)}, {"seq": lax.rem(z + S - 1, S)}]
    greeted += [{"fsdp": lax.rem(x + 1, X)}, {"fsdp": lax.rem(x + X - 1, X)}, {"sub": other}]
    for device in greeted:
        pl.semaphore_signal(barrier, inc=1, device_id=device, device_id_type=MESH)

    get_tokens = pltpu.make_async_copy(tokens.at[rows(x, R)], tokv, lsem.at[0])
    get_value = pltpu.make_async_copy(wv.at[:, mine], W.at[rows(x, vd)], lsem.at[1])
    get_out = pltpu.make_async_copy(wo, WO.at[0], lsem.at[2])
    get_tab = pltpu.make_async_copy(qtab.at[c], qtabv, lsem.at[3])
    get_pick = pltpu.make_async_copy(pick.at[c], pickv, lsem.at[4])
    get_tokens.start()
    get_value.start()
    get_out.start()
    get_tab.start()
    get_pick.start()

    qkown[...] = jnp.zeros_like(qkown)
    for head in range(2):
        @pl.when(c == head)
        def _():
            base = 2 * fd * head
            qkown[base : base + fd, :] = wq[...].astype(f32)
            qkown[base + fd : base + 2 * fd, :] = wk[...].astype(f32)

    get_tokens.wait()
    chunk = min(1024, D)

    def squares(i, total):
        part = tokv[:, pl.ds(pl.multiple_of(i * chunk, chunk), chunk)].astype(f32)
        return total + jnp.sum(part * part, axis=1, keepdims=True)

    meansq = lax.fori_loop(0, D // chunk, squares, jnp.zeros((R, 1), f32)) / D
    scale = lax.rsqrt(meansq + 1e-05)
    chunk = min(1024, Dh)

    @pl.loop(0, Dh // chunk)
    def _(i):
        here = pl.ds(pl.multiple_of(c * Dh + i * chunk, chunk), chunk)
        part = tokv[:, here].astype(f32) * scale * gain[:, here]
        T[0, :, pl.ds(pl.multiple_of(i * chunk, chunk), chunk)] = part.astype(bf16)

    pl.semaphore_wait(barrier, len(greeted))

    half = R // 2
    token_ring = Ring("seq", S, z, lambda p, way, step, b: T.at[slot_of(S, way, step), half * p : half * (p + 1)], 2, 1, tS, tR)
    token_ring.first()

    give_value = remote(wv.at[:, theirs], W.at[pl.ds(pl.multiple_of(HD + x * vd, vd), vd)], pS.at[0], pR.at[0], sub=other)
    give_qk = remote(qkown.at[:, theirs], qkin, pS.at[1], pR.at[1], sub=other)
    give_value.start()
    give_qk.start()

    def weight_piece(p, way, step, b):
        if p == 2:
            return QKf.at[rows(b, 4 * fd)]
        return W.at[pl.ds(pl.multiple_of(HD * p + b * vd, vd), vd)]

    weight_ring = Ring("fsdp", X, x, weight_piece, 3, 1, wS, wR)
    get_value.wait()
    give_value.wait_recv()
    give_qk.wait_recv()
    QKf[rows(x, 4 * fd), :] = qkown[:, mine] + qkin[...]
    weight_ring.first()

    W[2 * HD + 4 * count :, :] = jnp.zeros((W.shape[0] - 2 * HD - 4 * count, Dh), bf16)
    for g in range(S // GROUP):
        VBD[g] = jnp.zeros(VBD.shape[1:], bf16)
    Sg[:, FEATURES:, :] = jnp.zeros((S, 2 * LANES - FEATURES, HD), bf16)

    out_ring = Ring("seq", S, z, lambda p, way, step, b: WO.at[slot_of(S, way, step), HD * p : HD * (p + 1)], 2, 1, oS, oR)

    def swaps(n):
        first, slots = sets[n]
        here = slice(first * R, (first + slots) * R)
        return (remote(Pn.at[here, HD : 2 * HD + LANES], Rn.at[here], e2S.at[n, 0], e2R.at[n, 0], sub=other),
                remote(PT.at[:, here], RT.at[:, here], e2S.at[n, 1], e2R.at[n, 1], sub=other))

    def project(n):
        first, slots = sets[n]
        for j in range(first, first + slots, GROUP):
            lhs = T[j : j + GROUP].reshape(GROUP * R, Dh)
            here = slice(j * R, (j + GROUP) * R)
            Pn[here, :] = nt(lhs, W[...])
            PT[:, here] = nt(W[2 * HD : 2 * HD + 4 * count, :], lhs)
        for copy in swaps(n):
            copy.start()

    def gather_piece(n):
        first, slots = sets[n]

        def piece(p, way, step, b):
            if p == 0:
                return Vp.at[b, first : first + slots]
            return Kg.at[first // GROUP : (first + slots) // GROUP, :, rows(b, LANES)]

        return piece

    gather = [Ring("fsdp", X, x, gather_piece(n), 2, 1, kS.at[n], kR.at[n]) for n in range(len(sets))]

    def combine(n):
        first, slots = sets[n]
        here = slice(first * R, (first + slots) * R)
        for copy in swaps(n):
            copy.wait_recv()
        Vp[x, first : first + slots] = (Pn[here, :HD] + Rn[here, :HD]).astype(bf16).reshape(slots, R, HD)
        entries = (PT[:, here] + RT[:, here]).astype(bf16)
        keys = mm(pickv[...], entries).astype(bf16)
        for g in range(slots // GROUP):
            Kg[first // GROUP + g, :, rows(x, LANES)] = keys[:, g * LANES : (g + 1) * LANES]
        gather[n].first()
        Qn[here, :] = (Pn[here, 2 * HD :] + Rn[here, HD:]).astype(bf16)

    row = lax.broadcasted_iota(jnp.int32, (GROUP * R, X * LANES), 0)
    key = lax.broadcasted_iota(jnp.int32, (GROUP * R, X * LANES), 1)
    seen = (key // LANES) * R + key % R <= x * R + row % R
    lane = lax.broadcasted_iota(jnp.int32, (GROUP * R, LANES), 1)

    def within(g):
        keys = Kg[g]
        feats = ((mm(ktab[0], keys) + upright[0][:, :1]) * (mm(ktab[1], keys) + upright[1][:, :1])).astype(bf16)
        for b in range(X):
            for i in range(GROUP):
                VBD[g, b * LANES + i * R : b * LANES + (i + 1) * R, i * HD : (i + 1) * HD] = Vp[b, GROUP * g + i]
        spread = VBD[g]
        contrib = mm(feats, spread)
        for i in range(GROUP):
            Cs[GROUP * g + i] = contrib[:, i * HD : (i + 1) * HD]
        entries = Qn[g * GROUP * R : (g + 1) * GROUP * R, :]
        query_feats = ((mm(entries, qtabv[0]) + bias[0:1, :]) * (mm(entries, qtabv[1]) + bias[1:2, :])).astype(bf16)
        Fq[g] = query_feats
        line = jnp.where(lane <= count, query_feats[:, :LANES], jnp.zeros((GROUP * R, LANES), bf16))
        s = mm(line, feats[:LANES])
        weight = jnp.where(seen, 0.5 * (s * s) + 0.5, 0.0).astype(bf16)
        near = mm(weight, spread)
        for i in range(GROUP):
            num[g, i * R : (i + 1) * R, :] = near[i * R : (i + 1) * R, i * HD : (i + 1) * HD]

    jobs = [(5.6 * s, 0, functools.partial(token_ring.tick, s)) for s in range(1, S // 2 + 1)]
    jobs += [(3.0 + 8.0 * s, 1, functools.partial(weight_ring.tick, s)) for s in range(1, X // 2 + 1)]
    weights_at = 3.0 + 8.0 * (X // 2)

    def keep_qk():
        W[2 * HD : 2 * HD + 4 * count, :] = QKf[...].astype(bf16)

    jobs.append((weights_at + 0.1, 2, keep_qk))

    def out_first():
        get_out.wait()
        out_ring.first()

    jobs.append((5.6 * (S // 2) - 0.5, 2, out_first))
    now = weights_at
    for n, (first, slots) in enumerate(sets):
        last = first + slots - 1
        now = max(now + 1.0, 5.6 * ((last + 1) // 2))
        jobs.append((now + 0.2, 2, functools.partial(project, n)))
        jobs.append((now + 3.0, 2, functools.partial(combine, n)))
        for step in range(1, X // 2 + 1):
            jobs.append((now + 3.0 + 2.2 * step, 2, functools.partial(gather[n].tick, step)))
        for g in range(first // GROUP, (first + slots) // GROUP):
            jobs.append((now + 4.0 + 2.2 * (X // 2) + 0.1 * g, 2, functools.partial(within, g)))
        now = now + 3.0
    jobs += [(5.6 * (S // 2 + s), 0, functools.partial(out_ring.tick, s)) for s in range(1, min(2, S // 2 - 1) + 1)]

    get_tab.wait()
    get_pick.wait()
    for _, _, job in sorted(jobs, key=lambda j: j[:2]):
        job()
    done = min(2, S // 2 - 1)

    def prefix(p, total):
        away = lax.rem(p + S - z, S)
        slot = 2 * away + (away // (S // 2)) * (2 * S - 1 - 4 * away)
        Sg[slot, :FEATURES, :] = total.astype(bf16)
        return total + Cs[slot]

    lax.fori_loop(0, S, prefix, jnp.zeros((FEATURES, HD), f32))

    for g in range(S // GROUP):
        states = jnp.concatenate([Sg[GROUP * g + i] for i in range(GROUP)], axis=1)
        far = mm(Fq[g], states)
        for i in range(GROUP):
            here = slice(i * R, (i + 1) * R)
            widened = (num[g, here, :] + far[here, i * HD : (i + 1) * HD]).astype(bf16).astype(f32)
            power = jnp.mean(widened * widened, axis=1, keepdims=True)
            A1[GROUP * g + i] = (widened * lax.rsqrt(power + 1e-06) * hgain[...]).astype(bf16)

    lanes = pl.ds(pl.multiple_of(c * HD, LANES), HD)

    def to_plane(k):
        up, down = (slot_of(S, 1, k), slot_of(S, 0, k)) if k <= S // 2 else (slot_of(S, 0, S - k), slot_of(S, 1, S - k))
        return remote(A1.at[up], Att.at[down, rows(x, R), lanes], zS.at[k], zR.at[k], seq=lax.rem(z + k, S))

    far_first = sorted(range(1, S), key=lambda k: -min(k, S - k))
    for k in far_first:
        to_plane(k).start()
    Att[0, rows(x, R), lanes] = A1[0]

    upper = S // 2

    def share(p, way, step, b):
        return Att.at[upper * p : upper * (p + 1), rows(b, R), lanes]

    def relay(way, step, p, b):
        ref = share(p, way, step, b)
        return remote(ref, ref, relS.at[way, step - 1, p], relR.at[way, step - 1, p], sub=other)

    def own_relay(p):
        ref = share(p, 0, 0, x)
        return remote(ref, ref, ownS.at[p], ownR.at[p], sub=other)

    share_ring = Ring("fsdp", X, x, share, 2, 1, aS, aR)

    def arrive(p):
        for k in far_first:
            down = slot_of(S, 0, k) if k <= S // 2 else slot_of(S, 1, S - k)
            if down // upper == p:
                to_plane(k).wait_recv()
        share_ring.first([p])
        own_relay(p).start()

    def service():
        nonlocal done
        if done < S // 2 - 1:
            done += 1
            out_ring.tick(done)

    service()
    arrive(0)
    arrive(1)
    service()
    for step in range(1, X // 2 + 1):
        share_ring.tick(step, lambda way, s, p, b: relay(way, s, p, b).start())
        if step % 2 == 1:
            service()

    for p in range(2):
        own_relay(p).wait_recv()
    for step in range(1, X // 2 + 1):
        for p in range(2):
            for way in range(2):
                if share_ring.moves(way, step, p):
                    relay(way, step, p, share_ring.block(way, step)).wait_recv()

    acc[...] = mm(Att[0], WO[0])

    def add(j):
        acc[...] += mm(Att[j], WO[j])

    @pl.loop(1, 2 * done + 1)
    def _(j):
        add(j)

    while done < S // 2 - 1:
        service()
        add(2 * done - 1)
        add(2 * done)
    out_ring.tick(S // 2)
    out[...] = (acc[...] + mm(Att[S - 1], WO[S - 1])).astype(bf16)

    token_ring.drain()
    weight_ring.drain()
    out_ring.drain()
    share_ring.drain()
    for ring in gather:
        ring.drain()
    give_value.wait_send()
    give_qk.wait_send()
    for n in range(len(sets)):
        for copy in swaps(n):
            copy.wait_send()
    for k in range(1, S):
        to_plane(k).wait_send()
    for p in range(2):
        own_relay(p).wait_send()
    for step in range(1, X // 2 + 1):
        for p in range(2):
            for way in range(2):
                if share_ring.moves(way, step, p):
                    relay(way, step, p, x).wait_send()


def solution(mesh):
    S, X = mesh.shape["seq"], mesh.shape["fsdp"]
    if S >= 16:
        sets = [(0, S // 2)] + [(first, GROUP) for first in range(S // 2, S, GROUP)]
    else:
        sets = [(first, GROUP) for first in range(0, S, GROUP)]

    def per_device(tokens, norm_gain, w_query, w_key, w_value, head_gain, w_out):
        Ppl, D = tokens.shape
        fd, vd = w_query.shape[1], w_value.shape[1]
        HD, R, Dh, C = X * vd, Ppl // X, D // 2, w_out.shape[2]
        count, groups = X * fd, S // GROUP
        qtab, pick, ktab, bias, upright = feature_tables(X, fd)
        any_ref = pl.BlockSpec(memory_space=pl.ANY)
        vm = pl.BlockSpec(memory_space=pltpu.VMEM)
        dma = pltpu.SemaphoreType.DMA
        V = pltpu.VMEM
        scratch = [
            V((R, D), bf16),
            V((S, R, Dh), bf16),
            V((2 * HD + LANES, Dh), bf16),
            V((4 * count, Dh), f32),
            V((4 * fd, D), f32),
            V((4 * fd, Dh), f32),
            V((S * R, 2 * HD + LANES), f32),
            V((S * R, HD + LANES), f32),
            V((4 * count, S * R), f32),
            V((4 * count, S * R), f32),
            V((S * R, LANES), bf16),
            V((X, S, R, HD), bf16),
            V((groups, count, X * LANES), bf16),
            V((groups, X * LANES, GROUP * HD), bf16),
            V((S, FEATURES, HD), f32),
            V((S, 2 * LANES, HD), bf16),
            V((groups, GROUP * R, 2 * LANES), bf16),
            V((groups, GROUP * R, HD), f32),
            V((S, R, HD), bf16),
            V((S, Ppl, 2 * HD), bf16),
            V((S, 2 * HD, C), bf16),
            V((Ppl, C), f32),
            V((2, LANES, 2 * LANES), bf16),
            V((count, 4 * count), bf16),
            dma((5,)),
            dma((2, S // 2, 2)), dma((2, S // 2, 2)),
            dma((2, X // 2, 3)), dma((2, X // 2, 3)),
            dma((2, S // 2, 2)), dma((2, S // 2, 2)),
            dma((2, X // 2, 2)), dma((2, X // 2, 2)),
            dma((len(sets), 2, X // 2, 2)), dma((len(sets), 2, X // 2, 2)),
            dma((2,)), dma((2,)),
            dma((len(sets), 2)), dma((len(sets), 2)),
            dma((S,)), dma((S,)),
            dma((2,)), dma((2,)),
            dma((2, X // 2, 2)), dma((2, X // 2, 2)),
        ]
        return pl.pallas_call(
            functools.partial(layer, S, X, sets),
            out_shape=jax.ShapeDtypeStruct((Ppl, C), bf16),
            in_specs=[any_ref, vm, vm, vm, any_ref, vm, any_ref, any_ref, any_ref, vm, vm, vm],
            out_specs=vm,
            scratch_shapes=scratch,
            compiler_params=pltpu.CompilerParams(
                collective_id=0, has_side_effects=True, vmem_limit_bytes=67043328),
            name="layer",
        )(
            tokens,
            norm_gain.reshape(1, D),
            w_query.reshape(fd, D),
            w_key.reshape(fd, D),
            w_value.reshape(vd, D),
            head_gain.reshape(1, HD),
            w_out.reshape(2 * HD, C),
            qtab,
            pick,
            ktab,
            bias,
            upright,
        )

    in_specs = (
        P(("groups", "seq"), None),
        P(),
        P(("seq", "sub"), "fsdp", None),
        P(("seq", "sub"), "fsdp", None),
        P(("seq", "sub"), "fsdp", None),
        P(),
        P("seq", None, ("fsdp", "sub")),
    )
    out_specs = P(("groups", "seq"), ("fsdp", "sub"))
    return jax.shard_map(
        per_device, mesh=mesh, in_specs=in_specs, out_specs=out_specs, check_vma=False
    )
```

```python
import functools

import jax
import jax.numpy as jnp
import numpy as np
from jax import lax
from jax.experimental import pallas as pl
from jax.experimental.pallas import tpu as pltpu
from jax.sharding import PartitionSpec as P

LANES = 128
FEATURES = 160
GROUP = 4
MESH = pl.DeviceIdType.MESH
bf16, f32 = jnp.bfloat16, jnp.float32


def feature_tables(owners, dims):
    count = owners * dims
    queries = np.zeros((2, 2, LANES, 2 * LANES), np.float32)
    pick = np.zeros((2, count, 4 * count), np.float32)
    keys = np.zeros((2, FEATURES, count), np.float32)
    bias = np.zeros((8, 2 * LANES), np.float32)

    def entry(i, head, kind):
        return (i // dims) * 4 * dims + head * 2 * dims + kind * dims + i % dims

    for i in range(count):
        keys[0, i, i] = 0.5
        for head in range(2):
            queries[head, 0, entry(i, head, 0), i] = 0.5
            pick[head, i, entry(i, head, 1)] = 1.0
    feature = count + 1
    for i in range(count):
        for j in range(i, count):
            keys[0, feature, i] = 0.125 if i == j else 0.25
            keys[1, feature, j] = 1.0
            for head in range(2):
                queries[head, 0, entry(i, head, 0), feature] = 0.25
                queries[head, 1, entry(j, head, 0), feature] = 1.0
            feature += 1
    bias[0, count] = 1.0
    bias[1, : count + 1] = 1.0
    upright = np.zeros((2, FEATURES, LANES), np.float32)
    upright[0], upright[1] = bias[0, :FEATURES, None], bias[1, :FEATURES, None]
    return (jnp.asarray(queries, bf16), jnp.asarray(pick, bf16), jnp.asarray(keys, bf16),
            jnp.asarray(bias, f32), jnp.asarray(upright, f32))


class Ring:
    def __init__(self, axis, size, me, piece, pieces, split, send, recv):
        self.axis, self.size, self.me = axis, size, me
        self.piece, self.pieces, self.split = piece, pieces, split
        self.send, self.recv, self.last = send, recv, size // 2

    def moves(self, way, step, p):
        return step < self.last or (p < self.split) == (way == 0)

    def block(self, way, back):
        return lax.rem(self.me + (self.size - back if way == 0 else back), self.size)

    def copy(self, way, step, p, src, dst):
        to = lax.rem(self.me + (1 if way == 0 else self.size - 1), self.size)
        return pltpu.make_async_remote_copy(
            src_ref=src,
            dst_ref=dst,
            send_sem=self.send.at[way, step - 1, p],
            recv_sem=self.recv.at[way, step - 1, p],
            device_id={self.axis: to},
            device_id_type=MESH,
        )

    def start(self, way, step, p):
        if step <= self.last and self.moves(way, step, p):
            block = self.block(way, step - 1)
            self.copy(way, step, p, self.piece(p, way, step - 1, block), self.piece(p, way, step, block)).start()

    def first(self, pieces=None):
        for p in range(self.pieces) if pieces is None else pieces:
            for way in range(2):
                self.start(way, 1, p)

    def tick(self, step, p, arrived=None):
        for way in range(2):
            if self.moves(way, step, p):
                block = self.block(way, step)
                ref = self.piece(p, way, step, block)
                self.copy(way, step, p, ref, ref).wait_recv()
                self.start(way, step + 1, p)
                if arrived is not None:
                    arrived(way, step, p, block)

    def drain(self):
        for step in range(1, self.last + 1):
            for p in range(self.pieces):
                for way in range(2):
                    if self.moves(way, step, p):
                        ref = self.piece(p, way, step - 1, self.me)
                        self.copy(way, step, p, ref, ref).wait_send()


def nt(a, b):
    return lax.dot_general(a, b, (((1,), (1,)), ((), ())), preferred_element_type=f32)


def mm(a, b):
    return jnp.dot(a, b, preferred_element_type=f32)


def slot_of(size, way, step):
    if step == 0:
        return 0
    return size - 1 if step == size // 2 else 2 * step - 1 + way


def layer(S, X, sets, tokens, gain_hbm, wq_hbm, wk_hbm, wv, hgain_hbm, wo, qtab, pick, ktab_hbm, bias_hbm, upright_hbm, out,
          gain, wq, wk, hgain, ktab, bias, upright, tokv, T, W, QKf, QKb, qkown, qkin, Pn, Rn, PT, RT, Qn, Vp, Kg, VBD, Cs, Sg, Fq, num, A1, Att, WO, acc, qtabv, pickv,
          lsem, tS, tR, wS, wR, oS, oR, aS, aR, kS, kR, dS, dR, pS, pR, e2S, e2R, zS, zR, ownS, ownR, relS, relR):
    x, z, c = lax.axis_index("fsdp"), lax.axis_index("seq"), lax.axis_index("sub")
    R, D = tokv.shape
    Dh = D // 2
    vd, fd = wv.shape[0], wq.shape[0]
    HD = X * vd
    count = X * fd
    other = 1 - c
    mine = pl.ds(pl.multiple_of(c * Dh, LANES), Dh)
    theirs = pl.ds(pl.multiple_of(other * Dh, LANES), Dh)

    def rows(i, n):
        return pl.ds(pl.multiple_of(i * n, n), n)

    def remote(src, dst, send, recv, **device):
        return pltpu.make_async_remote_copy(
            src_ref=src, dst_ref=dst, send_sem=send, recv_sem=recv, device_id=device, device_id_type=MESH)

    barrier = pltpu.get_barrier_semaphore()
    greeted = [{"seq": lax.rem(z + 1, S)}, {"seq": lax.rem(z + S - 1, S)}]
    greeted += [{"fsdp": lax.rem(x + 1, X)}, {"fsdp": lax.rem(x + X - 1, X)}, {"sub": other}]
    for device in greeted:
        pl.semaphore_signal(barrier, inc=1, device_id=device, device_id_type=MESH)

    get_tokens = pltpu.make_async_copy(tokens.at[rows(x, R)], tokv, lsem.at[0])
    get_value = pltpu.make_async_copy(wv.at[:, mine], W.at[rows(x, vd)], lsem.at[1])
    get_out = pltpu.make_async_copy(wo, WO.at[0], lsem.at[2])
    get_tab = pltpu.make_async_copy(qtab.at[c], qtabv, lsem.at[3])
    get_pick = pltpu.make_async_copy(pick.at[c], pickv, lsem.at[4])
    small = [(gain_hbm, gain), (wq_hbm, wq), (wk_hbm, wk), (hgain_hbm, hgain), (ktab_hbm, ktab), (bias_hbm, bias), (upright_hbm, upright)]
    get_gain, get_wq, get_wk, *get_later = [
        pltpu.make_async_copy(src, dst, lsem.at[5 + i]) for i, (src, dst) in enumerate(small)]
    get_later += [get_tab, get_pick]
    for copy in [get_tokens, get_gain, get_wq, get_wk, get_value, get_out] + get_later:
        copy.start()

    get_tokens.wait()
    chunk = min(1024, D)

    def squares(i, total):
        part = tokv[:, pl.ds(pl.multiple_of(i * chunk, chunk), chunk)].astype(f32)
        return total + jnp.sum(part * part, axis=1, keepdims=True)

    meansq = lax.fori_loop(0, D // chunk, squares, jnp.zeros((R, 1), f32)) / D
    scale = lax.rsqrt(meansq + 1e-05)
    chunk = min(1024, Dh)

    get_gain.wait()

    @pl.loop(0, Dh // chunk)
    def _(i):
        here = pl.ds(pl.multiple_of(c * Dh + i * chunk, chunk), chunk)
        part = tokv[:, here].astype(f32) * scale * gain[:, here]
        T[0, :, pl.ds(pl.multiple_of(i * chunk, chunk), chunk)] = part.astype(bf16)

    pl.semaphore_wait(barrier, len(greeted))

    half = R // 2
    token_ring = Ring("seq", S, z, lambda p, way, step, b: T.at[slot_of(S, way, step), half * p : half * (p + 1)], 2, 1, tS, tR)
    token_ring.first()

    get_wq.wait()
    get_wk.wait()
    qkown[...] = jnp.zeros_like(qkown)
    for head in range(2):
        @pl.when(c == head)
        def _():
            base = 2 * fd * head
            qkown[base : base + fd, :] = wq[...].astype(f32)
            qkown[base + fd : base + 2 * fd, :] = wk[...].astype(f32)

    give_value = remote(wv.at[:, theirs], W.at[pl.ds(pl.multiple_of(HD + x * vd, vd), vd)], pS.at[0], pR.at[0], sub=other)
    give_qk = remote(qkown.at[:, theirs], qkin, pS.at[1], pR.at[1], sub=other)
    give_value.start()
    give_qk.start()

    def weight_piece(p, way, step, b):
        if p == 2:
            return QKb.at[b]
        return W.at[pl.ds(pl.multiple_of(HD * p + b * vd, vd), vd)]

    weight_ring = Ring("fsdp", X, x, weight_piece, 3, 1, wS, wR)
    get_value.wait()
    give_value.wait_recv()
    give_qk.wait_recv()
    QKb[x] = (qkown[:, mine] + qkin[...]).astype(bf16)
    weight_ring.first()

    W[2 * HD + 4 * count :, :] = jnp.zeros((W.shape[0] - 2 * HD - 4 * count, Dh), bf16)
    for g in range(S // GROUP):
        VBD[g] = jnp.zeros(VBD.shape[1:], bf16)
    Sg[:, FEATURES:, :] = jnp.zeros((S, 2 * LANES - FEATURES, HD), bf16)

    out_ring = Ring("seq", S, z, lambda p, way, step, b: WO.at[slot_of(S, way, step), HD * p : HD * (p + 1)], 2, 1, oS, oR)

    def swaps(n):
        first, slots = sets[n]
        here = slice(first * R, (first + slots) * R)
        return (remote(Pn.at[here, HD : 2 * HD + LANES], Rn.at[here], e2S.at[n, 0], e2R.at[n, 0], sub=other),
                remote(PT.at[:, here], RT.at[:, here], e2S.at[n, 1], e2R.at[n, 1], sub=other))

    def project(n):
        first, slots = sets[n]
        for j in range(first, first + slots, GROUP):
            lhs = T[j : j + GROUP].reshape(GROUP * R, Dh)
            here = slice(j * R, (j + GROUP) * R)
            Pn[here, :] = nt(lhs, W[...])
            PT[:, here] = nt(W[2 * HD : 2 * HD + 4 * count, :], lhs)
        for copy in swaps(n):
            copy.start()

    def gather_piece(n):
        first, slots = sets[n]

        def piece(p, way, step, b):
            if p == 0:
                return Vp.at[b, first : first + slots]
            return Kg.at[first // GROUP : (first + slots) // GROUP, :, rows(b, LANES)]

        return piece

    gather = Ring("fsdp", X, x, gather_piece(0), 2, 1, kS, kR)
    nearest_last = sorted(range(1, X), key=lambda k: -min(k, X - k))

    def direct(n, k, p, owner):
        ref = gather_piece(n)(p, 0, 0, owner)
        return remote(ref, ref, dS.at[n, k, p], dR.at[n, k, p], fsdp=lax.rem(x + k, X))

    def combine(n):
        first, slots = sets[n]
        here = slice(first * R, (first + slots) * R)
        for copy in swaps(n):
            copy.wait_recv()
        Vp[x, first : first + slots] = (Pn[here, :HD] + Rn[here, :HD]).astype(bf16).reshape(slots, R, HD)
        entries = (PT[:, here] + RT[:, here]).astype(bf16)
        keys = mm(pickv[...], entries).astype(bf16)
        for g in range(slots // GROUP):
            Kg[first // GROUP + g, :, rows(x, LANES)] = keys[:, g * LANES : (g + 1) * LANES]
        if n == 0:
            gather.first()
        else:
            for k in nearest_last:
                for p in range(2):
                    direct(n, k, p, x).start()
        Qn[here, :] = (Pn[here, 2 * HD :] + Rn[here, HD:]).astype(bf16)

    row = lax.broadcasted_iota(jnp.int32, (GROUP * R, X * LANES), 0)
    key = lax.broadcasted_iota(jnp.int32, (GROUP * R, X * LANES), 1)
    seen = (key // LANES) * R + key % R <= x * R + row % R
    lane = lax.broadcasted_iota(jnp.int32, (GROUP * R, LANES), 1)

    def within(g):
        keys = Kg[g]
        feats = ((mm(ktab[0], keys) + upright[0][:, :1]) * (mm(ktab[1], keys) + upright[1][:, :1])).astype(bf16)
        for b in range(X):
            for i in range(GROUP):
                VBD[g, b * LANES + i * R : b * LANES + (i + 1) * R, i * HD : (i + 1) * HD] = Vp[b, GROUP * g + i]
        spread = VBD[g]
        contrib = mm(feats, spread)
        for i in range(GROUP):
            Cs[GROUP * g + i] = contrib[:, i * HD : (i + 1) * HD]
        entries = Qn[g * GROUP * R : (g + 1) * GROUP * R, :]
        query_feats = ((mm(entries, qtabv[0]) + bias[0:1, :]) * (mm(entries, qtabv[1]) + bias[1:2, :])).astype(bf16)
        Fq[g] = query_feats
        line = jnp.where(lane <= count, query_feats[:, :LANES], jnp.zeros((GROUP * R, LANES), bf16))
        s = mm(line, feats[:LANES])
        weight = jnp.where(seen, 0.5 * (s * s) + 0.5, 0.0).astype(bf16)
        near = mm(weight, spread)
        for i in range(GROUP):
            num[g, i * R : (i + 1) * R, :] = near[i * R : (i + 1) * R, i * HD : (i + 1) * HD]

    def keep_qk():
        for b in range(X):
            QKf[4 * fd * b : 4 * fd * (b + 1), :] = QKb[b].astype(f32)
        W[2 * HD : 2 * HD + 4 * count, :] = QKf[...].astype(bf16)

    def out_first():
        get_out.wait()
        out_ring.first()

    def landed(n):
        for k in nearest_last:
            for p in range(2):
                direct(n, k, p, lax.rem(x + X - k, X)).wait_recv()

    def prefix(p, total):
        away = lax.rem(p + S - z, S)
        slot = 2 * away + (away // (S // 2)) * (2 * S - 1 - 4 * away)
        Sg[slot, :FEATURES, :] = total.astype(bf16)
        return total + Cs[slot]

    lanes = pl.ds(pl.multiple_of(c * HD, LANES), HD)

    def to_plane(k):
        up, down = (slot_of(S, 1, k), slot_of(S, 0, k)) if k <= S // 2 else (slot_of(S, 0, S - k), slot_of(S, 1, S - k))
        return remote(A1.at[up], Att.at[down, rows(x, R), lanes], zS.at[k], zR.at[k], seq=lax.rem(z + k, S))

    far_first = sorted(range(1, S), key=lambda k: -min(k, S - k))

    def attend():
        lax.fori_loop(0, S, prefix, jnp.zeros((FEATURES, HD), f32))
        for g in range(S // GROUP):
            states = jnp.concatenate([Sg[GROUP * g + i] for i in range(GROUP)], axis=1)
            far = mm(Fq[g], states)
            for i in range(GROUP):
                here = slice(i * R, (i + 1) * R)
                widened = (num[g, here, :] + far[here, i * HD : (i + 1) * HD]).astype(bf16).astype(f32)
                power = jnp.mean(widened * widened, axis=1, keepdims=True)
                A1[GROUP * g + i] = (widened * lax.rsqrt(power + 1e-06) * hgain[...]).astype(bf16)
        for k in far_first:
            to_plane(k).start()
        Att[0, rows(x, R), lanes] = A1[0]

    quarter = S // GROUP

    def share(p, way, step, b):
        return Att.at[GROUP * p : GROUP * (p + 1), rows(b, R), lanes]

    def relay(way, step, p, b):
        ref = share(p, way, step, b)
        return remote(ref, ref, relS.at[way, step - 1, p], relR.at[way, step - 1, p], sub=other)

    def own_relay(p):
        ref = share(p, 0, 0, x)
        return remote(ref, ref, ownS.at[p], ownR.at[p], sub=other)

    share_ring = Ring("fsdp", X, x, share, quarter, quarter // 2, aS, aR)

    def arrive(p):
        for k in far_first:
            down = slot_of(S, 0, k) if k <= S // 2 else slot_of(S, 1, S - k)
            if down // GROUP == p:
                to_plane(k).wait_recv()
        share_ring.first([p])
        own_relay(p).start()

    def spread(step, p):
        share_ring.tick(step, p, lambda way, s, p, b: relay(way, s, p, b).start())

    def whole(p):
        own_relay(p).wait_recv()
        for step in range(1, X // 2 + 1):
            for way in range(2):
                if share_ring.moves(way, step, p):
                    relay(way, step, p, share_ring.block(way, step)).wait_recv()

    def product(first, last):
        lhs = jnp.concatenate([Att[j] for j in range(first, last)], axis=1)
        term = mm(lhs, WO[first:last].reshape((last - first) * 2 * HD, WO.shape[2]))
        if last == S:
            out[...] = (acc[...] + term).astype(bf16)
        else:
            acc[...] = term if first == 0 else acc[...] + term

    jobs = []

    def at(time, job, *details):
        jobs.append((time, len(jobs), functools.partial(job, *details)))

    half_z, half_x = S // 2, X // 2
    for step in range(1, half_z + 1):
        for p in range(2):
            at(9.5 + 5.9 * (step - 1) + 2.95 * (p + 1), token_ring.tick, step, p)
    for step in range(1, half_x + 1):
        for p in range(3):
            at(9.5 + 7.2 * (step - 1) + 2.4 * (p + 1), weight_ring.tick, step, p)
    held = 9.6 + 7.2 * half_x
    turn = 9.5 + 5.9 * half_z
    at(turn - 5.8, out_first)
    at(held, keep_qk)
    free = held
    for n, (first, slots) in enumerate(sets):
        last = 9.6 + 5.9 * ((first + slots) // 2)
        start = max(free, last)
        at(start, project, n)
        at(start + 4.0, combine, n)
        if n == 0:
            for step in range(1, half_x + 1):
                for p in range(2):
                    at(start + 4.0 + 3.2 * (step - 1) + 1.6 * (p + 1), gather.tick, step, p)
            end = start + 4.2 + 3.2 * half_x
        else:
            end = start + 12.5
            at(end, landed, n)
        for g in range(first // GROUP, (first + slots) // GROUP):
            at(end + 0.1, within, g)
        free = start + 4.1
    at(end + 1.0, attend)
    for p in range(quarter):
        at(end + 9.0 + 0.7 * p, arrive, p)
    for step in range(1, half_x + 1):
        for p in range(quarter):
            at(end + 11.0 + 3.2 * (step - 1) + 0.8 * (p + 1), spread, step, p)
    for p in range(quarter):
        time = end + 12.0 + 3.2 * half_x + 0.5 * p
        at(time, whole, p)
        ready = turn + 5.7 * min(2 * p + 2, half_z - 1) + 0.1
        at(max(time, ready), product, GROUP * p, min(GROUP * (p + 1), S - 1))
    at(max(time, turn + 5.7 * half_z) + 0.2, product, S - 1, S)
    for step in range(1, half_z + 1):
        for p in range(2):
            at(turn + 5.7 * (step - 1) + 2.85 * (p + 1), out_ring.tick, step, p)

    for copy in get_later:
        copy.wait()
    for _, _, job in sorted(jobs, key=lambda job: job[:2]):
        job()

    token_ring.drain()
    weight_ring.drain()
    out_ring.drain()
    share_ring.drain()
    gather.drain()
    for n in range(1, len(sets)):
        for k in range(1, X):
            for p in range(2):
                direct(n, k, p, x).wait_send()
    give_value.wait_send()
    give_qk.wait_send()
    for n in range(len(sets)):
        for copy in swaps(n):
            copy.wait_send()
    for k in range(1, S):
        to_plane(k).wait_send()
    for p in range(quarter):
        own_relay(p).wait_send()
    for step in range(1, X // 2 + 1):
        for p in range(quarter):
            for way in range(2):
                if share_ring.moves(way, step, p):
                    relay(way, step, p, x).wait_send()


def solution(mesh):
    S, X = mesh.shape["seq"], mesh.shape["fsdp"]
    early = max(S // 2, GROUP)
    sets = [(0, early)] + [(first, GROUP) for first in range(early, S, GROUP)]

    def per_device(tokens, norm_gain, w_query, w_key, w_value, head_gain, w_out):
        Ppl, D = tokens.shape
        fd, vd = w_query.shape[1], w_value.shape[1]
        HD, R, Dh, C = X * vd, Ppl // X, D // 2, w_out.shape[2]
        count, groups = X * fd, S // GROUP
        qtab, pick, ktab, bias, upright = feature_tables(X, fd)
        in_hbm = pl.BlockSpec(memory_space=pltpu.MemorySpace.HBM)
        vm = pl.BlockSpec(memory_space=pltpu.VMEM)
        dma = pltpu.SemaphoreType.DMA
        V = pltpu.VMEM
        scratch = [
            V((1, D), f32),
            V((fd, D), bf16),
            V((fd, D), bf16),
            V((1, HD), f32),
            V((2, FEATURES, count), bf16),
            V((8, 2 * LANES), f32),
            V((2, FEATURES, LANES), f32),
            V((R, D), bf16),
            V((S, R, Dh), bf16),
            V((2 * HD + LANES, Dh), bf16),
            V((4 * count, Dh), f32),
            V((X, 4 * fd, Dh), bf16),
            V((4 * fd, D), f32),
            V((4 * fd, Dh), f32),
            V((S * R, 2 * HD + LANES), f32),
            V((S * R, HD + LANES), f32),
            V((4 * count, S * R), f32),
            V((4 * count, S * R), f32),
            V((S * R, LANES), bf16),
            V((X, S, R, HD), bf16),
            V((groups, count, X * LANES), bf16),
            V((groups, X * LANES, GROUP * HD), bf16),
            V((S, FEATURES, HD), f32),
            V((S, 2 * LANES, HD), bf16),
            V((groups, GROUP * R, 2 * LANES), bf16),
            V((groups, GROUP * R, HD), f32),
            V((S, R, HD), bf16),
            V((S, Ppl, 2 * HD), bf16),
            V((S, 2 * HD, C), bf16),
            V((Ppl, C), f32),
            V((2, LANES, 2 * LANES), bf16),
            V((count, 4 * count), bf16),
            dma((12,)),
            dma((2, S // 2, 2)), dma((2, S // 2, 2)),
            dma((2, X // 2, 3)), dma((2, X // 2, 3)),
            dma((2, S // 2, 2)), dma((2, S // 2, 2)),
            dma((2, X // 2, groups)), dma((2, X // 2, groups)),
            dma((2, X // 2, 2)), dma((2, X // 2, 2)),
            dma((len(sets), X, 2)), dma((len(sets), X, 2)),
            dma((2,)), dma((2,)),
            dma((len(sets), 2)), dma((len(sets), 2)),
            dma((S,)), dma((S,)),
            dma((groups,)), dma((groups,)),
            dma((2, X // 2, groups)), dma((2, X // 2, groups)),
        ]
        return pl.pallas_call(
            functools.partial(layer, S, X, sets),
            out_shape=jax.ShapeDtypeStruct((Ppl, C), bf16),
            in_specs=[in_hbm] * 12,
            out_specs=vm,
            scratch_shapes=scratch,
            compiler_params=pltpu.CompilerParams(
                collective_id=0, has_side_effects=True, vmem_limit_bytes=56 * 1024 * 1024),
            name="layer",
        )(
            tokens,
            norm_gain.reshape(1, D),
            w_query.reshape(fd, D),
            w_key.reshape(fd, D),
            w_value.reshape(vd, D),
            head_gain.reshape(1, HD),
            w_out.reshape(2 * HD, C),
            qtab,
            pick,
            ktab,
            bias,
            upright,
        )

    in_specs = (
        P(("groups", "seq"), None),
        P(),
        P(("seq", "sub"), "fsdp", None),
        P(("seq", "sub"), "fsdp", None),
        P(("seq", "sub"), "fsdp", None),
        P(),
        P("seq", None, ("fsdp", "sub")),
    )
    out_specs = P(("groups", "seq"), ("fsdp", "sub"))
    return jax.shard_map(
        per_device, mesh=mesh, in_specs=in_specs, out_specs=out_specs, check_vma=False
    )
```

```python
import functools

import jax
import jax.numpy as jnp
import numpy as np
from jax import lax
from jax.experimental import pallas as pl
from jax.experimental.pallas import tpu as pltpu
from jax.sharding import PartitionSpec as P

LANES = 128
FEATURES = 160
GROUP = 4
MESH = pl.DeviceIdType.MESH
bf16, f32 = jnp.bfloat16, jnp.float32


def feature_tables(owners, dims):
    count = owners * dims
    queries = np.zeros((2, 2, LANES, 2 * LANES), np.float32)
    pick = np.zeros((2, count, 4 * count), np.float32)
    keys = np.zeros((2, FEATURES, count), np.float32)
    bias = np.zeros((8, 2 * LANES), np.float32)

    def entry(i, head, kind):
        return (i // dims) * 4 * dims + head * 2 * dims + kind * dims + i % dims

    for i in range(count):
        keys[0, i, i] = 0.5
        for head in range(2):
            queries[head, 0, entry(i, head, 0), i] = 0.5
            pick[head, i, entry(i, head, 1)] = 1.0
    feature = count + 1
    for i in range(count):
        for j in range(i, count):
            keys[0, feature, i] = 0.125 if i == j else 0.25
            keys[1, feature, j] = 1.0
            for head in range(2):
                queries[head, 0, entry(i, head, 0), feature] = 0.25
                queries[head, 1, entry(j, head, 0), feature] = 1.0
            feature += 1
    bias[0, count] = 1.0
    bias[1, : count + 1] = 1.0
    upright = np.zeros((2, FEATURES, LANES), np.float32)
    upright[0], upright[1] = bias[0, :FEATURES, None], bias[1, :FEATURES, None]
    return (jnp.asarray(queries, bf16), jnp.asarray(pick, bf16), jnp.asarray(keys, bf16),
            jnp.asarray(bias, f32), jnp.asarray(upright, f32))


class Ring:
    def __init__(self, axis, size, me, piece, pieces, split, send, recv):
        self.axis, self.size, self.me = axis, size, me
        self.piece, self.pieces, self.split = piece, pieces, split
        self.send, self.recv, self.last = send, recv, size // 2

    def moves(self, way, step, p):
        return step < self.last or (p < self.split) == (way == 0)

    def block(self, way, back):
        return lax.rem(self.me + (self.size - back if way == 0 else back), self.size)

    def copy(self, way, step, p, src, dst):
        to = lax.rem(self.me + (1 if way == 0 else self.size - 1), self.size)
        return pltpu.make_async_remote_copy(
            src_ref=src,
            dst_ref=dst,
            send_sem=self.send.at[way, step - 1, p],
            recv_sem=self.recv.at[way, step - 1, p],
            device_id={self.axis: to},
            device_id_type=MESH,
        )

    def start(self, way, step, p):
        if step <= self.last and self.moves(way, step, p):
            block = self.block(way, step - 1)
            self.copy(way, step, p, self.piece(p, way, step - 1, block), self.piece(p, way, step, block)).start()

    def first(self, pieces=None):
        for p in range(self.pieces) if pieces is None else pieces:
            for way in range(2):
                self.start(way, 1, p)

    def tick(self, step, p, arrived=None):
        for way in range(2):
            if self.moves(way, step, p):
                block = self.block(way, step)
                ref = self.piece(p, way, step, block)
                self.copy(way, step, p, ref, ref).wait_recv()
                self.start(way, step + 1, p)
                if arrived is not None:
                    arrived(way, step, p, block)

    def drain(self):
        for step in range(1, self.last + 1):
            for p in range(self.pieces):
                for way in range(2):
                    if self.moves(way, step, p):
                        ref = self.piece(p, way, step - 1, self.me)
                        self.copy(way, step, p, ref, ref).wait_send()


def nt(a, b):
    return lax.dot_general(a, b, (((1,), (1,)), ((), ())), preferred_element_type=f32)


def mm(a, b):
    return jnp.dot(a, b, preferred_element_type=f32)


def slot_of(size, way, step):
    if step == 0:
        return 0
    return size - 1 if step == size // 2 else 2 * step - 1 + way


def layer(S, X, sets, tokens, gain_hbm, wq_hbm, wk_hbm, wv, hgain_hbm, wo, qtab, pick, ktab_hbm, bias_hbm, upright_hbm, out,
          gain, wq, wk, hgain, ktab, bias, upright, tokv, T, W, QKf, QKb, qkown, qkin, Pn, Rn, PT, RT, Qn, Vp, Kg, VBD, Cs, Sg, Fq, num, A1, Att, WO, acc, qtabv, pickv,
          lsem, tS, tR, wS, wR, oS, oR, aS, aR, kS, kR, dS, dR, pS, pR, e2S, e2R, zS, zR, ownS, ownR, relS, relR):
    x, z, c = lax.axis_index("fsdp"), lax.axis_index("seq"), lax.axis_index("sub")
    R, D = tokv.shape
    Dh = D // 2
    vd, fd = wv.shape[0], wq.shape[0]
    HD = X * vd
    count = X * fd
    other = 1 - c
    mine = pl.ds(pl.multiple_of(c * Dh, LANES), Dh)
    theirs = pl.ds(pl.multiple_of(other * Dh, LANES), Dh)

    def rows(i, n):
        return pl.ds(pl.multiple_of(i * n, n), n)

    def remote(src, dst, send, recv, **device):
        return pltpu.make_async_remote_copy(
            src_ref=src, dst_ref=dst, send_sem=send, recv_sem=recv, device_id=device, device_id_type=MESH)

    barrier = pltpu.get_barrier_semaphore()
    greeted = [{"seq": lax.rem(z + 1, S)}, {"seq": lax.rem(z + S - 1, S)}]
    greeted += [{"fsdp": lax.rem(x + 1, X)}, {"fsdp": lax.rem(x + X - 1, X)}, {"sub": other}]
    for device in greeted:
        pl.semaphore_signal(barrier, inc=1, device_id=device, device_id_type=MESH)

    half = R // 2
    get_tokens = [
        pltpu.make_async_copy(
            tokens.at[pl.ds(pl.multiple_of(x * R + half * p, half), half)], tokv.at[half * p : half * (p + 1)], lsem.at[12 + p])
        for p in range(2)
    ]
    get_value = pltpu.make_async_copy(wv.at[:, mine], W.at[rows(x, vd)], lsem.at[1])
    get_out = pltpu.make_async_copy(wo, WO.at[0], lsem.at[2])
    get_tab = pltpu.make_async_copy(qtab.at[c], qtabv, lsem.at[3])
    get_pick = pltpu.make_async_copy(pick.at[c], pickv, lsem.at[4])
    small = [(gain_hbm, gain), (wq_hbm, wq), (wk_hbm, wk), (hgain_hbm, hgain), (ktab_hbm, ktab), (bias_hbm, bias), (upright_hbm, upright)]
    get_gain, get_wq, get_wk, *get_later = [
        pltpu.make_async_copy(src, dst, lsem.at[5 + i]) for i, (src, dst) in enumerate(small)]
    get_later += [get_tab, get_pick]
    for copy in get_tokens + [get_gain, get_wq, get_wk, get_value, get_out] + get_later:
        copy.start()

    get_wq.wait()
    get_wk.wait()
    qkown[...] = jnp.zeros_like(qkown)
    for head in range(2):
        @pl.when(c == head)
        def _():
            base = 2 * fd * head
            qkown[base : base + fd, :] = wq[...].astype(f32)
            qkown[base + fd : base + 2 * fd, :] = wk[...].astype(f32)

    pl.semaphore_wait(barrier, len(greeted))
    give_value = remote(wv.at[:, theirs], W.at[pl.ds(pl.multiple_of(HD + x * vd, vd), vd)], pS.at[0], pR.at[0], sub=other)
    give_qk = remote(qkown.at[:, theirs], qkin, pS.at[1], pR.at[1], sub=other)
    give_value.start()
    give_qk.start()

    def token_piece(p, way, step, b):
        up, side = divmod(p, 2)
        return T.at[slot_of(S, way, step), half * up : half * (up + 1), Dh // 2 * side : Dh // 2 * (side + 1)]

    token_ring = Ring("seq", S, z, token_piece, 4, 2, tS, tR)
    chunk, piece = min(1024, D), min(1024, Dh)
    get_gain.wait()
    for p in range(2):
        part = slice(half * p, half * (p + 1))
        get_tokens[p].wait()

        def squares(i, total):
            values = tokv[part, pl.ds(pl.multiple_of(i * chunk, chunk), chunk)].astype(f32)
            return total + jnp.sum(values * values, axis=1, keepdims=True)

        meansq = lax.fori_loop(0, D // chunk, squares, jnp.zeros((half, 1), f32)) / D
        scale = lax.rsqrt(meansq + 1e-05)

        @pl.loop(0, Dh // piece)
        def _(i):
            here = pl.ds(pl.multiple_of(c * Dh + i * piece, piece), piece)
            values = tokv[part, here].astype(f32) * scale * gain[:, here]
            T[0, part, pl.ds(pl.multiple_of(i * piece, piece), piece)] = values.astype(bf16)

        token_ring.first([2 * p, 2 * p + 1])

    def weight_piece(p, way, step, b):
        if p == 2:
            return QKb.at[b]
        return W.at[pl.ds(pl.multiple_of(HD * p + b * vd, vd), vd)]

    weight_ring = Ring("fsdp", X, x, weight_piece, 3, 1, wS, wR)
    get_value.wait()
    give_value.wait_recv()
    give_qk.wait_recv()
    QKb[x] = (qkown[:, mine] + qkin[...]).astype(bf16)
    weight_ring.first()

    W[2 * HD + 4 * count :, :] = jnp.zeros((W.shape[0] - 2 * HD - 4 * count, Dh), bf16)
    for g in range(S // GROUP):
        VBD[g] = jnp.zeros(VBD.shape[1:], bf16)
    Sg[:, FEATURES:, :] = jnp.zeros((S, 2 * LANES - FEATURES, HD), bf16)

    out_ring = Ring("seq", S, z, lambda p, way, step, b: WO.at[slot_of(S, way, step), HD // 2 * p : HD // 2 * (p + 1)], 4, 2, oS, oR)

    def swaps(n):
        first, slots = sets[n]
        here = slice(first * R, (first + slots) * R)
        return (remote(Pn.at[here, HD : 2 * HD + LANES], Rn.at[here], e2S.at[n, 0], e2R.at[n, 0], sub=other),
                remote(PT.at[:, here], RT.at[:, here], e2S.at[n, 1], e2R.at[n, 1], sub=other))

    def project(n, j):
        first, slots = sets[n]
        lhs = T[j : j + GROUP].reshape(GROUP * R, Dh)
        here = slice(j * R, (j + GROUP) * R)
        Pn[here, :] = nt(lhs, W[...])
        PT[:, here] = nt(W[2 * HD : 2 * HD + 4 * count, :], lhs)
        if j + GROUP == first + slots:
            for copy in swaps(n):
                copy.start()

    def gather_piece(n):
        first, slots = sets[n]

        def piece(p, way, step, b):
            if p == 0:
                return Vp.at[b, first : first + slots]
            return Kg.at[first // GROUP : (first + slots) // GROUP, :, rows(b, LANES)]

        return piece

    gather = Ring("fsdp", X, x, gather_piece(0), 2, 1, kS, kR)
    nearest_last = sorted(range(1, X), key=lambda k: -min(k, X - k))

    def direct(n, k, p, owner):
        ref = gather_piece(n)(p, 0, 0, owner)
        return remote(ref, ref, dS.at[n, k, p], dR.at[n, k, p], fsdp=lax.rem(x + k, X))

    def combine(n):
        first, slots = sets[n]
        here = slice(first * R, (first + slots) * R)
        for copy in swaps(n):
            copy.wait_recv()
        Vp[x, first : first + slots] = (Pn[here, :HD] + Rn[here, :HD]).astype(bf16).reshape(slots, R, HD)
        entries = (PT[:, here] + RT[:, here]).astype(bf16)
        keys = mm(pickv[...], entries).astype(bf16)
        for g in range(slots // GROUP):
            Kg[first // GROUP + g, :, rows(x, LANES)] = keys[:, g * LANES : (g + 1) * LANES]
        if n == 0:
            gather.first()
        else:
            for k in nearest_last:
                for p in range(2):
                    direct(n, k, p, x).start()
        Qn[here, :] = (Pn[here, 2 * HD :] + Rn[here, HD:]).astype(bf16)

    row = lax.broadcasted_iota(jnp.int32, (GROUP * R, X * LANES), 0)
    key = lax.broadcasted_iota(jnp.int32, (GROUP * R, X * LANES), 1)
    seen = (key // LANES) * R + key % R <= x * R + row % R
    lane = lax.broadcasted_iota(jnp.int32, (GROUP * R, LANES), 1)

    def within(g):
        keys = Kg[g]
        feats = ((mm(ktab[0], keys) + upright[0][:, :1]) * (mm(ktab[1], keys) + upright[1][:, :1])).astype(bf16)
        for b in range(X):
            for i in range(GROUP):
                VBD[g, b * LANES + i * R : b * LANES + (i + 1) * R, i * HD : (i + 1) * HD] = Vp[b, GROUP * g + i]
        spread = VBD[g]
        contrib = mm(feats, spread)
        for i in range(GROUP):
            Cs[GROUP * g + i] = contrib[:, i * HD : (i + 1) * HD]
        entries = Qn[g * GROUP * R : (g + 1) * GROUP * R, :]
        query_feats = ((mm(entries, qtabv[0]) + bias[0:1, :]) * (mm(entries, qtabv[1]) + bias[1:2, :])).astype(bf16)
        Fq[g] = query_feats
        line = jnp.where(lane <= count, query_feats[:, :LANES], jnp.zeros((GROUP * R, LANES), bf16))
        s = mm(line, feats[:LANES])
        weight = jnp.where(seen, 0.5 * (s * s) + 0.5, 0.0).astype(bf16)
        near = mm(weight, spread)
        for i in range(GROUP):
            num[g, i * R : (i + 1) * R, :] = near[i * R : (i + 1) * R, i * HD : (i + 1) * HD]

    def keep_qk():
        for b in range(X):
            QKf[4 * fd * b : 4 * fd * (b + 1), :] = QKb[b].astype(f32)
        W[2 * HD : 2 * HD + 4 * count, :] = QKf[...].astype(bf16)

    def out_first():
        get_out.wait()
        out_ring.first()

    def landed(n):
        for k in nearest_last:
            for p in range(2):
                direct(n, k, p, lax.rem(x + X - k, X)).wait_recv()

    def prefix(p, total):
        away = lax.rem(p + S - z, S)
        slot = 2 * away + (away // (S // 2)) * (2 * S - 1 - 4 * away)
        Sg[slot, :FEATURES, :] = total.astype(bf16)
        return total + Cs[slot]

    lanes = pl.ds(pl.multiple_of(c * HD, LANES), HD)

    def to_plane(k):
        up, down = (slot_of(S, 1, k), slot_of(S, 0, k)) if k <= S // 2 else (slot_of(S, 0, S - k), slot_of(S, 1, S - k))
        return remote(A1.at[up], Att.at[down, rows(x, R), lanes], zS.at[k], zR.at[k], seq=lax.rem(z + k, S))

    outward = sorted(range(1, S), key=lambda k: -min(k, S - k))

    def attend():
        lax.fori_loop(0, S, prefix, jnp.zeros((FEATURES, HD), f32))
        for g in range(S // GROUP):
            states = jnp.concatenate([Sg[GROUP * g + i] for i in range(GROUP)], axis=1)
            far = mm(Fq[g], states)
            for i in range(GROUP):
                here = slice(i * R, (i + 1) * R)
                widened = (num[g, here, :] + far[here, i * HD : (i + 1) * HD]).astype(bf16).astype(f32)
                power = jnp.mean(widened * widened, axis=1, keepdims=True)
                A1[GROUP * g + i] = (widened * lax.rsqrt(power + 1e-06) * hgain[...]).astype(bf16)
        for k in outward:
            to_plane(k).start()
        Att[0, rows(x, R), lanes] = A1[0]

    quarter = S // GROUP

    def share(p, way, step, b):
        return Att.at[GROUP * p : GROUP * (p + 1), rows(b, R), lanes]

    def relay(way, step, p, b):
        ref = share(p, way, step, b)
        return remote(ref, ref, relS.at[way, step - 1, p], relR.at[way, step - 1, p], sub=other)

    def own_relay(p):
        ref = share(p, 0, 0, x)
        return remote(ref, ref, ownS.at[p], ownR.at[p], sub=other)

    share_ring = Ring("fsdp", X, x, share, quarter, quarter // 2, aS, aR)

    def arrive(p):
        for k in outward:
            down = slot_of(S, 0, k) if k <= S // 2 else slot_of(S, 1, S - k)
            if down // GROUP == p:
                to_plane(k).wait_recv()
        share_ring.first([p])
        own_relay(p).start()

    def spread(step, p):
        share_ring.tick(step, p, lambda way, s, p, b: relay(way, s, p, b).start())

    def whole(p):
        own_relay(p).wait_recv()
        for step in range(1, X // 2 + 1):
            for way in range(2):
                if share_ring.moves(way, step, p):
                    relay(way, step, p, share_ring.block(way, step)).wait_recv()

    def product(first, last):
        lhs = jnp.concatenate([Att[j] for j in range(first, last)], axis=1)
        term = mm(lhs, WO[first:last].reshape((last - first) * 2 * HD, WO.shape[2]))
        if last == S:
            out[...] = (acc[...] + term).astype(bf16)
        else:
            acc[...] = term if first == 0 else acc[...] + term

    jobs = []

    def at(time, job, *details):
        jobs.append((time, len(jobs), functools.partial(job, *details)))

    half_z, half_x = S // 2, X // 2
    step_z, step_x, step_o = 5.9, 8.0, 5.2
    for step in range(1, half_z + 1):
        for p in range(4):
            at(9.5 + step_z * (step - 1) + step_z / 4 * (p + 1), token_ring.tick, step, p)
    for step in range(1, half_x + 1):
        for p in range(3):
            at(9.5 + step_x * (step - 1) + step_x / 3 * (p + 1), weight_ring.tick, step, p)
    held = 9.6 + step_x * half_x
    turn = 9.5 + step_z * half_z
    at(turn - 5.8, out_first)
    at(held, keep_qk)
    free = held
    for n, (first, slots) in enumerate(sets):
        last = 9.6 + step_z * ((first + slots) // 2)
        start = max(free, last)
        final = n == len(sets) - 1
        for j in range(first, first + slots, GROUP):
            at(start + 1.4 * (j - first) / GROUP, project, n, j)
        joined = start + (3.2 if final else 5.6)
        at(joined, combine, n)
        if n == 0:
            for step in range(1, half_x + 1):
                for p in range(2):
                    at(joined + 3.8 * step + 0.8 * p, gather.tick, step, p)
            end = joined + 3.8 * half_x + 1.0
        else:
            end = joined + (8.8 if final else 11.5)
            at(end, landed, n)
        for g in range(first // GROUP, (first + slots) // GROUP):
            at(end + 0.1, within, g)
        free = start + 1.5 * slots / GROUP
    at(end + 1.0, attend)
    for p in range(quarter):
        at(end + 9.0 + 0.7 * p, arrive, p)
    for step in range(1, half_x + 1):
        for p in range(quarter):
            at(end + 11.0 + 3.2 * (step - 1) + 0.8 * (p + 1), spread, step, p)
    for p in range(quarter):
        time = end + 12.0 + 3.2 * half_x + 0.5 * p
        at(time, whole, p)
        ready = turn + step_o * min(2 * p + 2, half_z - 1) + 0.1
        at(max(time, ready), product, GROUP * p, min(GROUP * (p + 1), S - 1))
    at(max(time, turn + step_o * half_z) + 0.2, product, S - 1, S)
    for step in range(1, half_z + 1):
        for p in range(4):
            at(turn + step_o * (step - 1) + step_o / 4 * (p + 1), out_ring.tick, step, p)

    for copy in get_later:
        copy.wait()
    for _, _, job in sorted(jobs, key=lambda job: job[:2]):
        job()

    token_ring.drain()
    weight_ring.drain()
    out_ring.drain()
    share_ring.drain()
    gather.drain()
    for n in range(1, len(sets)):
        for k in range(1, X):
            for p in range(2):
                direct(n, k, p, x).wait_send()
    give_value.wait_send()
    give_qk.wait_send()
    for n in range(len(sets)):
        for copy in swaps(n):
            copy.wait_send()
    for k in range(1, S):
        to_plane(k).wait_send()
    for p in range(quarter):
        own_relay(p).wait_send()
    for step in range(1, X // 2 + 1):
        for p in range(quarter):
            for way in range(2):
                if share_ring.moves(way, step, p):
                    relay(way, step, p, x).wait_send()


def solution(mesh):
    S, X = mesh.shape["seq"], mesh.shape["fsdp"]
    early = max(S // 2, GROUP)
    sets = [(0, early)] + [(first, GROUP) for first in range(early, S, GROUP)]

    def per_device(tokens, norm_gain, w_query, w_key, w_value, head_gain, w_out):
        Ppl, D = tokens.shape
        fd, vd = w_query.shape[1], w_value.shape[1]
        HD, R, Dh, C = X * vd, Ppl // X, D // 2, w_out.shape[2]
        count, groups = X * fd, S // GROUP
        qtab, pick, ktab, bias, upright = feature_tables(X, fd)
        in_hbm = pl.BlockSpec(memory_space=pltpu.MemorySpace.HBM)
        vm = pl.BlockSpec(memory_space=pltpu.VMEM)
        dma = pltpu.SemaphoreType.DMA
        V = pltpu.VMEM
        scratch = [
            V((1, D), f32),
            V((fd, D), bf16),
            V((fd, D), bf16),
            V((1, HD), f32),
            V((2, FEATURES, count), bf16),
            V((8, 2 * LANES), f32),
            V((2, FEATURES, LANES), f32),
            V((R, D), bf16),
            V((S, R, Dh), bf16),
            V((2 * HD + LANES, Dh), bf16),
            V((4 * count, Dh), f32),
            V((X, 4 * fd, Dh), bf16),
            V((4 * fd, D), f32),
            V((4 * fd, Dh), f32),
            V((S * R, 2 * HD + LANES), f32),
            V((S * R, HD + LANES), f32),
            V((4 * count, S * R), f32),
            V((4 * count, S * R), f32),
            V((S * R, LANES), bf16),
            V((X, S, R, HD), bf16),
            V((groups, count, X * LANES), bf16),
            V((groups, X * LANES, GROUP * HD), bf16),
            V((S, FEATURES, HD), f32),
            V((S, 2 * LANES, HD), bf16),
            V((groups, GROUP * R, 2 * LANES), bf16),
            V((groups, GROUP * R, HD), f32),
            V((S, R, HD), bf16),
            V((S, Ppl, 2 * HD), bf16),
            V((S, 2 * HD, C), bf16),
            V((Ppl, C), f32),
            V((2, LANES, 2 * LANES), bf16),
            V((count, 4 * count), bf16),
            dma((14,)),
            dma((2, S // 2, 4)), dma((2, S // 2, 4)),
            dma((2, X // 2, 3)), dma((2, X // 2, 3)),
            dma((2, S // 2, 4)), dma((2, S // 2, 4)),
            dma((2, X // 2, groups)), dma((2, X // 2, groups)),
            dma((2, X // 2, 2)), dma((2, X // 2, 2)),
            dma((len(sets), X, 2)), dma((len(sets), X, 2)),
            dma((2,)), dma((2,)),
            dma((len(sets), 2)), dma((len(sets), 2)),
            dma((S,)), dma((S,)),
            dma((groups,)), dma((groups,)),
            dma((2, X // 2, groups)), dma((2, X // 2, groups)),
        ]
        return pl.pallas_call(
            functools.partial(layer, S, X, sets),
            out_shape=jax.ShapeDtypeStruct((Ppl, C), bf16),
            in_specs=[in_hbm] * 12,
            out_specs=vm,
            scratch_shapes=scratch,
            compiler_params=pltpu.CompilerParams(
                collective_id=0, has_side_effects=True, vmem_limit_bytes=56 * 1024 * 1024),
            name="layer",
        )(
            tokens,
            norm_gain.reshape(1, D),
            w_query.reshape(fd, D),
            w_key.reshape(fd, D),
            w_value.reshape(vd, D),
            head_gain.reshape(1, HD),
            w_out.reshape(2 * HD, C),
            qtab,
            pick,
            ktab,
            bias,
            upright,
        )

    in_specs = (
        P(("groups", "seq"), None),
        P(),
        P(("seq", "sub"), "fsdp", None),
        P(("seq", "sub"), "fsdp", None),
        P(("seq", "sub"), "fsdp", None),
        P(),
        P("seq", None, ("fsdp", "sub")),
    )
    out_specs = P(("groups", "seq"), ("fsdp", "sub"))
    return jax.shard_map(
        per_device, mesh=mesh, in_specs=in_specs, out_specs=out_specs, check_vma=False
    )
```

```python
import functools

import jax
import jax.numpy as jnp
import numpy as np
from jax import lax
from jax.experimental import pallas as pl
from jax.experimental.pallas import tpu as pltpu
from jax.sharding import PartitionSpec as P

LANES = 128
FEATURES = 160
GROUP = 4
MESH = pl.DeviceIdType.MESH
bf16, f32 = jnp.bfloat16, jnp.float32


def feature_tables(owners, dims):
    count = owners * dims
    queries = np.zeros((2, 2, LANES, 2 * LANES), np.float32)
    pick = np.zeros((2, count, 4 * count), np.float32)
    keys = np.zeros((2, FEATURES, count), np.float32)
    bias = np.zeros((8, 2 * LANES), np.float32)

    def entry(i, head, kind):
        return (i // dims) * 4 * dims + head * 2 * dims + kind * dims + i % dims

    for i in range(count):
        keys[0, i, i] = 0.5
        for head in range(2):
            queries[head, 0, entry(i, head, 0), i] = 0.5
            pick[head, i, entry(i, head, 1)] = 1.0
    feature = count + 1
    for i in range(count):
        for j in range(i, count):
            keys[0, feature, i] = 0.125 if i == j else 0.25
            keys[1, feature, j] = 1.0
            for head in range(2):
                queries[head, 0, entry(i, head, 0), feature] = 0.25
                queries[head, 1, entry(j, head, 0), feature] = 1.0
            feature += 1
    bias[0, count] = 1.0
    bias[1, : count + 1] = 1.0
    upright = np.zeros((2, FEATURES, LANES), np.float32)
    upright[0], upright[1] = bias[0, :FEATURES, None], bias[1, :FEATURES, None]
    return (jnp.asarray(queries, bf16), jnp.asarray(pick, bf16), jnp.asarray(keys, bf16),
            jnp.asarray(bias, f32), jnp.asarray(upright, f32))


class Ring:
    def __init__(self, axis, size, me, piece, pieces, split, send, recv):
        self.axis, self.size, self.me = axis, size, me
        self.piece, self.pieces, self.split = piece, pieces, split
        self.send, self.recv, self.last = send, recv, size // 2

    def moves(self, way, step, p):
        return step < self.last or (p < self.split) == (way == 0)

    def block(self, way, back):
        return lax.rem(self.me + (self.size - back if way == 0 else back), self.size)

    def copy(self, way, step, p, src, dst):
        to = lax.rem(self.me + (1 if way == 0 else self.size - 1), self.size)
        return pltpu.make_async_remote_copy(
            src_ref=src,
            dst_ref=dst,
            send_sem=self.send.at[way, step - 1, p],
            recv_sem=self.recv.at[way, step - 1, p],
            device_id={self.axis: to},
            device_id_type=MESH,
        )

    def start(self, way, step, p):
        if step <= self.last and self.moves(way, step, p):
            block = self.block(way, step - 1)
            self.copy(way, step, p, self.piece(p, way, step - 1, block), self.piece(p, way, step, block)).start()

    def first(self, pieces=None):
        for p in range(self.pieces) if pieces is None else pieces:
            for way in range(2):
                self.start(way, 1, p)

    def tick(self, step, p, arrived=None):
        for way in range(2):
            if self.moves(way, step, p):
                block = self.block(way, step)
                ref = self.piece(p, way, step, block)
                self.copy(way, step, p, ref, ref).wait_recv()
                self.start(way, step + 1, p)
                if arrived is not None:
                    arrived(way, step, p, block)

    def drain(self):
        for step in range(1, self.last + 1):
            for p in range(self.pieces):
                for way in range(2):
                    if self.moves(way, step, p):
                        ref = self.piece(p, way, step - 1, self.me)
                        self.copy(way, step, p, ref, ref).wait_send()


def nt(a, b):
    return lax.dot_general(a, b, (((1,), (1,)), ((), ())), preferred_element_type=f32)


def mm(a, b):
    return jnp.dot(a, b, preferred_element_type=f32)


def slot_of(size, way, step):
    if step == 0:
        return 0
    return size - 1 if step == size // 2 else 2 * step - 1 + way


def layer(S, X, sets, tokens, gain_hbm, wq_hbm, wk_hbm, wv, hgain_hbm, wo, qtab, pick, ktab_hbm, bias_hbm, upright_hbm, out,
          gain, wq, wk, hgain, ktab, bias, upright, tokv, T, W, QKf, QKb, qkown, qkin, Pn, Rn, PT, RT, Qn, Vp, Kg, VBD, Cs, Sg, Fq, num, A1, Att, WO, acc, qtabv, pickv,
          lsem, tS, tR, wS, wR, oS, oR, aS, aR, kS, kR, dS, dR, pS, pR, e2S, e2R, zS, zR, ownS, ownR, relS, relR):
    x, z, c = lax.axis_index("fsdp"), lax.axis_index("seq"), lax.axis_index("sub")
    R, D = tokv.shape
    Dh = D // 2
    vd, fd = wv.shape[0], wq.shape[0]
    HD = X * vd
    count = X * fd
    other = 1 - c
    mine = pl.ds(pl.multiple_of(c * Dh, LANES), Dh)
    theirs = pl.ds(pl.multiple_of(other * Dh, LANES), Dh)

    def rows(i, n):
        return pl.ds(pl.multiple_of(i * n, n), n)

    def remote(src, dst, send, recv, **device):
        return pltpu.make_async_remote_copy(
            src_ref=src, dst_ref=dst, send_sem=send, recv_sem=recv, device_id=device, device_id_type=MESH)

    barrier = pltpu.get_barrier_semaphore()
    greeted = [{"seq": lax.rem(z + 1, S)}, {"seq": lax.rem(z + S - 1, S)}]
    greeted += [{"fsdp": lax.rem(x + 1, X)}, {"fsdp": lax.rem(x + X - 1, X)}, {"sub": other}]
    for device in greeted:
        pl.semaphore_signal(barrier, inc=1, device_id=device, device_id_type=MESH)

    half = R // 2
    get_tokens = [
        pltpu.make_async_copy(
            tokens.at[pl.ds(pl.multiple_of(x * R + half * p, half), half)], tokv.at[half * p : half * (p + 1)], lsem.at[12 + p])
        for p in range(2)
    ]
    get_value = pltpu.make_async_copy(wv.at[:, mine], W.at[rows(x, vd)], lsem.at[1])
    get_out = pltpu.make_async_copy(wo, WO.at[0], lsem.at[2])
    get_tab = pltpu.make_async_copy(qtab.at[c], qtabv, lsem.at[3])
    get_pick = pltpu.make_async_copy(pick.at[c], pickv, lsem.at[4])
    small = [(gain_hbm, gain), (wq_hbm, wq), (wk_hbm, wk), (hgain_hbm, hgain), (ktab_hbm, ktab), (bias_hbm, bias), (upright_hbm, upright)]
    get_gain, get_wq, get_wk, *get_later = [
        pltpu.make_async_copy(src, dst, lsem.at[5 + i]) for i, (src, dst) in enumerate(small)]
    get_later += [get_tab, get_pick]
    for copy in get_tokens + [get_gain, get_wq, get_wk, get_value, get_out] + get_later:
        copy.start()

    get_wq.wait()
    get_wk.wait()
    qkown[...] = jnp.zeros_like(qkown)
    for head in range(2):
        @pl.when(c == head)
        def _():
            base = 2 * fd * head
            qkown[base : base + fd, :] = wq[...].astype(f32)
            qkown[base + fd : base + 2 * fd, :] = wk[...].astype(f32)

    pl.semaphore_wait(barrier, len(greeted))
    give_value = remote(wv.at[:, theirs], W.at[pl.ds(pl.multiple_of(HD + x * vd, vd), vd)], pS.at[0], pR.at[0], sub=other)
    give_qk = remote(qkown.at[:, theirs], qkin, pS.at[1], pR.at[1], sub=other)
    give_value.start()
    give_qk.start()

    def token_piece(p, way, step, b):
        up, side = divmod(p, 2)
        return T.at[slot_of(S, way, step), half * up : half * (up + 1), Dh // 2 * side : Dh // 2 * (side + 1)]

    token_ring = Ring("seq", S, z, token_piece, 4, 2, tS, tR)
    chunk, piece = min(1024, D), min(1024, Dh)
    get_gain.wait()
    for p in range(2):
        part = slice(half * p, half * (p + 1))
        get_tokens[p].wait()

        def squares(i, total):
            values = tokv[part, pl.ds(pl.multiple_of(i * chunk, chunk), chunk)].astype(f32)
            return total + jnp.sum(values * values, axis=1, keepdims=True)

        meansq = lax.fori_loop(0, D // chunk, squares, jnp.zeros((half, 1), f32)) / D
        scale = lax.rsqrt(meansq + 1e-05)

        @pl.loop(0, Dh // piece)
        def _(i):
            here = pl.ds(pl.multiple_of(c * Dh + i * piece, piece), piece)
            values = tokv[part, here].astype(f32) * scale * gain[:, here]
            T[0, part, pl.ds(pl.multiple_of(i * piece, piece), piece)] = values.astype(bf16)

        token_ring.first([2 * p, 2 * p + 1])

    def weight_piece(p, way, step, b):
        if p == 2:
            return QKb.at[b]
        return W.at[pl.ds(pl.multiple_of(HD * p + b * vd, vd), vd)]

    weight_ring = Ring("fsdp", X, x, weight_piece, 3, 1, wS, wR)
    get_value.wait()
    give_value.wait_recv()
    give_qk.wait_recv()
    QKb[x] = (qkown[:, mine] + qkin[...]).astype(bf16)
    weight_ring.first()

    W[2 * HD + 4 * count :, :] = jnp.zeros((W.shape[0] - 2 * HD - 4 * count, Dh), bf16)
    for g in range(S // GROUP):
        VBD[g] = jnp.zeros(VBD.shape[1:], bf16)
    Sg[:, FEATURES:, :] = jnp.zeros((S, 2 * LANES - FEATURES, HD), bf16)

    out_ring = Ring("seq", S, z, lambda p, way, step, b: WO.at[slot_of(S, way, step), HD // 2 * p : HD // 2 * (p + 1)], 4, 2, oS, oR)

    def swaps(n):
        first, slots = sets[n]
        here = slice(first * R, (first + slots) * R)
        return (remote(Pn.at[here, HD : 2 * HD + LANES], Rn.at[here], e2S.at[n, 0], e2R.at[n, 0], sub=other),
                remote(PT.at[:, here], RT.at[:, here], e2S.at[n, 1], e2R.at[n, 1], sub=other))

    def project(n, j):
        first, slots = sets[n]
        lhs = T[j : j + GROUP].reshape(GROUP * R, Dh)
        here = slice(j * R, (j + GROUP) * R)
        Pn[here, :] = nt(lhs, W[...])
        PT[:, here] = nt(W[2 * HD : 2 * HD + 4 * count, :], lhs)
        if j + GROUP == first + slots:
            for copy in swaps(n):
                copy.start()

    def gather_piece(n):
        first, slots = sets[n]

        def piece(p, way, step, b):
            if p == 0:
                return Vp.at[b, first : first + slots]
            return Kg.at[first // GROUP : (first + slots) // GROUP, :, rows(b, LANES)]

        return piece

    gather = Ring("fsdp", X, x, gather_piece(0), 2, 1, kS, kR)
    nearest_last = sorted(range(1, X), key=lambda k: -min(k, X - k))

    def direct(n, k, p, owner):
        ref = gather_piece(n)(p, 0, 0, owner)
        return remote(ref, ref, dS.at[n, k, p], dR.at[n, k, p], fsdp=lax.rem(x + k, X))

    def combine(n):
        first, slots = sets[n]
        here = slice(first * R, (first + slots) * R)
        for copy in swaps(n):
            copy.wait_recv()
        Vp[x, first : first + slots] = (Pn[here, :HD] + Rn[here, :HD]).astype(bf16).reshape(slots, R, HD)
        entries = (PT[:, here] + RT[:, here]).astype(bf16)
        keys = mm(pickv[...], entries).astype(bf16)
        for g in range(slots // GROUP):
            Kg[first // GROUP + g, :, rows(x, LANES)] = keys[:, g * LANES : (g + 1) * LANES]
        if n == 0:
            gather.first()
        else:
            for k in nearest_last:
                for p in range(2):
                    direct(n, k, p, x).start()
        Qn[here, :] = (Pn[here, 2 * HD :] + Rn[here, HD:]).astype(bf16)

    row = lax.broadcasted_iota(jnp.int32, (GROUP * R, X * LANES), 0)
    key = lax.broadcasted_iota(jnp.int32, (GROUP * R, X * LANES), 1)
    seen = (key // LANES) * R + key % R <= x * R + row % R
    lane = lax.broadcasted_iota(jnp.int32, (GROUP * R, LANES), 1)

    def within(g):
        keys = Kg[g]
        feats = ((mm(ktab[0], keys) + upright[0][:, :1]) * (mm(ktab[1], keys) + upright[1][:, :1])).astype(bf16)
        for b in range(X):
            for i in range(GROUP):
                VBD[g, b * LANES + i * R : b * LANES + (i + 1) * R, i * HD : (i + 1) * HD] = Vp[b, GROUP * g + i]
        spread = VBD[g]
        contrib = mm(feats, spread)
        for i in range(GROUP):
            Cs[GROUP * g + i] = contrib[:, i * HD : (i + 1) * HD]
        entries = Qn[g * GROUP * R : (g + 1) * GROUP * R, :]
        query_feats = ((mm(entries, qtabv[0]) + bias[0:1, :]) * (mm(entries, qtabv[1]) + bias[1:2, :])).astype(bf16)
        Fq[g] = query_feats
        line = jnp.where(lane <= count, query_feats[:, :LANES], jnp.zeros((GROUP * R, LANES), bf16))
        s = mm(line, feats[:LANES])
        weight = jnp.where(seen, 0.5 * (s * s) + 0.5, 0.0).astype(bf16)
        near = mm(weight, spread)
        for i in range(GROUP):
            num[g, i * R : (i + 1) * R, :] = near[i * R : (i + 1) * R, i * HD : (i + 1) * HD]

    def keep_qk():
        for b in range(X):
            QKf[4 * fd * b : 4 * fd * (b + 1), :] = QKb[b].astype(f32)
        W[2 * HD : 2 * HD + 4 * count, :] = QKf[...].astype(bf16)

    def out_first():
        get_out.wait()
        out_ring.first()

    def landed(n):
        for k in nearest_last:
            for p in range(2):
                direct(n, k, p, lax.rem(x + X - k, X)).wait_recv()

    def prefix(p, total):
        away = lax.rem(p + S - z, S)
        slot = 2 * away + (away // (S // 2)) * (2 * S - 1 - 4 * away)
        Sg[slot, :FEATURES, :] = total.astype(bf16)
        return total + Cs[slot]

    lanes = pl.ds(pl.multiple_of(c * HD, LANES), HD)

    def to_plane(k):
        up, down = (slot_of(S, 1, k), slot_of(S, 0, k)) if k <= S // 2 else (slot_of(S, 0, S - k), slot_of(S, 1, S - k))
        return remote(A1.at[up], Att.at[down, rows(x, R), lanes], zS.at[k], zR.at[k], seq=lax.rem(z + k, S))

    outward = sorted(range(1, S), key=lambda k: -min(k, S - k))

    def attend():
        lax.fori_loop(0, S, prefix, jnp.zeros((FEATURES, HD), f32))
        for g in range(S // GROUP):
            states = jnp.concatenate([Sg[GROUP * g + i] for i in range(GROUP)], axis=1)
            far = mm(Fq[g], states)
            for i in range(GROUP):
                here = slice(i * R, (i + 1) * R)
                widened = (num[g, here, :] + far[here, i * HD : (i + 1) * HD]).astype(bf16).astype(f32)
                power = jnp.mean(widened * widened, axis=1, keepdims=True)
                A1[GROUP * g + i] = (widened * lax.rsqrt(power + 1e-06) * hgain[...]).astype(bf16)
        for k in outward:
            to_plane(k).start()
        Att[0, rows(x, R), lanes] = A1[0]

    quarter = S // GROUP

    def share(p, way, step, b):
        return Att.at[GROUP * p : GROUP * (p + 1), rows(b, R), lanes]

    def relay(way, step, p, b):
        ref = share(p, way, step, b)
        return remote(ref, ref, relS.at[way, step - 1, p], relR.at[way, step - 1, p], sub=other)

    def own_relay(p):
        ref = share(p, 0, 0, x)
        return remote(ref, ref, ownS.at[p], ownR.at[p], sub=other)

    share_ring = Ring("fsdp", X, x, share, quarter, quarter // 2, aS, aR)

    def arrive(p):
        for k in outward:
            down = slot_of(S, 0, k) if k <= S // 2 else slot_of(S, 1, S - k)
            if down // GROUP == p:
                to_plane(k).wait_recv()
        share_ring.first([p])
        own_relay(p).start()

    def spread(step, p):
        share_ring.tick(step, p, lambda way, s, p, b: relay(way, s, p, b).start())

    def whole(p):
        own_relay(p).wait_recv()
        for step in range(1, X // 2 + 1):
            for way in range(2):
                if share_ring.moves(way, step, p):
                    relay(way, step, p, share_ring.block(way, step)).wait_recv()

    def product(first, last):
        lhs = jnp.concatenate([Att[j] for j in range(first, last)], axis=1)
        term = mm(lhs, WO[first:last].reshape((last - first) * 2 * HD, WO.shape[2]))
        if last == S:
            out[...] = (acc[...] + term).astype(bf16)
        else:
            acc[...] = term if first == 0 else acc[...] + term

    jobs = []

    def at(time, job, *details):
        jobs.append((time, len(jobs), functools.partial(job, *details)))

    half_z, half_x = S // 2, X // 2
    step_z, step_x, step_o = 5.9, 8.0, 5.2
    for step in range(1, half_z + 1):
        for p in range(4):
            at(9.5 + step_z * (step - 1) + step_z / 4 * (p + 1), token_ring.tick, step, p)
    for step in range(1, half_x + 1):
        for p in range(3):
            at(9.5 + step_x * (step - 1) + step_x / 3 * (p + 1), weight_ring.tick, step, p)
    held = 9.6 + step_x * half_x
    turn = 9.5 + step_z * half_z
    at(turn - 8.7, out_first)
    at(held, keep_qk)
    free = held
    for n, (first, slots) in enumerate(sets):
        last = 9.6 + step_z * ((first + slots) // 2)
        start = max(free, last)
        final = n == len(sets) - 1
        for j in range(first, first + slots, GROUP):
            at(start + 1.4 * (j - first) / GROUP, project, n, j)
        joined = start + (3.2 if final else 5.6)
        at(joined, combine, n)
        if n == 0:
            for step in range(1, half_x + 1):
                for p in range(2):
                    at(joined + 3.8 * step + 0.8 * p, gather.tick, step, p)
            end = joined + 3.8 * half_x + 1.0
        else:
            end = joined + (8.8 if final else 11.5)
            at(end, landed, n)
        for g in range(first // GROUP, (first + slots) // GROUP):
            at(end + 0.1, within, g)
        free = start + 1.5 * slots / GROUP
    at(end + 1.0, attend)
    for p in range(quarter):
        at(end + 9.0 + 0.7 * p, arrive, p)
    for step in range(1, half_x + 1):
        for p in range(quarter):
            at(end + 11.0 + 3.2 * (step - 1) + 0.8 * (p + 1), spread, step, p)
    for p in range(quarter):
        time = end + 12.0 + 3.2 * half_x + 0.5 * p
        at(time, whole, p)
        ready = turn + step_o * min(2 * p + 2, half_z - 1) + 0.1
        at(max(time, ready), product, GROUP * p, min(GROUP * (p + 1), S - 1))
    at(max(time, turn + step_o * half_z) + 0.2, product, S - 1, S)
    for step in range(1, half_z + 1):
        for p in range(4):
            at(turn - 2.0 + step_o * (step - 1) + step_o / 4 * (p + 1), out_ring.tick, step, p)

    for copy in get_later:
        copy.wait()
    for _, _, job in sorted(jobs, key=lambda job: job[:2]):
        job()

    token_ring.drain()
    weight_ring.drain()
    out_ring.drain()
    share_ring.drain()
    gather.drain()
    for n in range(1, len(sets)):
        for k in range(1, X):
            for p in range(2):
                direct(n, k, p, x).wait_send()
    give_value.wait_send()
    give_qk.wait_send()
    for n in range(len(sets)):
        for copy in swaps(n):
            copy.wait_send()
    for k in range(1, S):
        to_plane(k).wait_send()
    for p in range(quarter):
        own_relay(p).wait_send()
    for step in range(1, X // 2 + 1):
        for p in range(quarter):
            for way in range(2):
                if share_ring.moves(way, step, p):
                    relay(way, step, p, x).wait_send()


def solution(mesh):
    S, X = mesh.shape["seq"], mesh.shape["fsdp"]
    early = max(S // 2, GROUP)
    sets = [(0, early)] + [(first, GROUP) for first in range(early, S, GROUP)]

    def per_device(tokens, norm_gain, w_query, w_key, w_value, head_gain, w_out):
        Ppl, D = tokens.shape
        fd, vd = w_query.shape[1], w_value.shape[1]
        HD, R, Dh, C = X * vd, Ppl // X, D // 2, w_out.shape[2]
        count, groups = X * fd, S // GROUP
        qtab, pick, ktab, bias, upright = feature_tables(X, fd)
        in_hbm = pl.BlockSpec(memory_space=pltpu.MemorySpace.HBM)
        vm = pl.BlockSpec(memory_space=pltpu.VMEM)
        dma = pltpu.SemaphoreType.DMA
        V = pltpu.VMEM
        scratch = [
            V((1, D), f32),
            V((fd, D), bf16),
            V((fd, D), bf16),
            V((1, HD), f32),
            V((2, FEATURES, count), bf16),
            V((8, 2 * LANES), f32),
            V((2, FEATURES, LANES), f32),
            V((R, D), bf16),
            V((S, R, Dh), bf16),
            V((2 * HD + LANES, Dh), bf16),
            V((4 * count, Dh), f32),
            V((X, 4 * fd, Dh), bf16),
            V((4 * fd, D), f32),
            V((4 * fd, Dh), f32),
            V((S * R, 2 * HD + LANES), f32),
            V((S * R, HD + LANES), f32),
            V((4 * count, S * R), f32),
            V((4 * count, S * R), f32),
            V((S * R, LANES), bf16),
            V((X, S, R, HD), bf16),
            V((groups, count, X * LANES), bf16),
            V((groups, X * LANES, GROUP * HD), bf16),
            V((S, FEATURES, HD), f32),
            V((S, 2 * LANES, HD), bf16),
            V((groups, GROUP * R, 2 * LANES), bf16),
            V((groups, GROUP * R, HD), f32),
            V((S, R, HD), bf16),
            V((S, Ppl, 2 * HD), bf16),
            V((S, 2 * HD, C), bf16),
            V((Ppl, C), f32),
            V((2, LANES, 2 * LANES), bf16),
            V((count, 4 * count), bf16),
            dma((14,)),
            dma((2, S // 2, 4)), dma((2, S // 2, 4)),
            dma((2, X // 2, 3)), dma((2, X // 2, 3)),
            dma((2, S // 2, 4)), dma((2, S // 2, 4)),
            dma((2, X // 2, groups)), dma((2, X // 2, groups)),
            dma((2, X // 2, 2)), dma((2, X // 2, 2)),
            dma((len(sets), X, 2)), dma((len(sets), X, 2)),
            dma((2,)), dma((2,)),
            dma((len(sets), 2)), dma((len(sets), 2)),
            dma((S,)), dma((S,)),
            dma((groups,)), dma((groups,)),
            dma((2, X // 2, groups)), dma((2, X // 2, groups)),
        ]
        return pl.pallas_call(
            functools.partial(layer, S, X, sets),
            out_shape=jax.ShapeDtypeStruct((Ppl, C), bf16),
            in_specs=[in_hbm] * 12,
            out_specs=vm,
            scratch_shapes=scratch,
            compiler_params=pltpu.CompilerParams(
                collective_id=0, has_side_effects=True, vmem_limit_bytes=56 * 1024 * 1024),
            name="layer",
        )(
            tokens,
            norm_gain.reshape(1, D),
            w_query.reshape(fd, D),
            w_key.reshape(fd, D),
            w_value.reshape(vd, D),
            head_gain.reshape(1, HD),
            w_out.reshape(2 * HD, C),
            qtab,
            pick,
            ktab,
            bias,
            upright,
        )

    in_specs = (
        P(("groups", "seq"), None),
        P(),
        P(("seq", "sub"), "fsdp", None),
        P(("seq", "sub"), "fsdp", None),
        P(("seq", "sub"), "fsdp", None),
        P(),
        P("seq", None, ("fsdp", "sub")),
    )
    out_specs = P(("groups", "seq"), ("fsdp", "sub"))
    return jax.shard_map(
        per_device, mesh=mesh, in_specs=in_specs, out_specs=out_specs, check_vma=False
    )
```
